1024 devices in a mesh: fsdp: 16 (over y, z_hi), rep: 64 (over z_lo, x, core).
Axes of the slice: x: 8, y: 8, z: 8 (z_hi: 2, z_lo: 4; z = z_hi * 4 + z_lo), core: 2. Of those that a mesh axis runs over, the one named last changes fastest.
Arguments:
- hidden_in: bfloat16 [262144, 2048], P(('fsdp', 'rep'))
- out_grad: bfloat16 [262144, 2048], P(('fsdp', 'rep')), may hold values from -6 to 6
- attn_saved: bfloat16 [262144, 256], P(('fsdp', 'rep')), may hold values from -6 to 6
- row_lse: float32 [262144, 2], P(('fsdp', 'rep')), may hold values from 2.5 to 6
- w_qkv: bfloat16 [2048, 512], P('fsdp'), may hold values from -0.125 to 0.125
- w_out_t: bfloat16 [2048, 256], P('fsdp'), may hold values from -0.125 to 0.125
- doc_lengths: int32 [1024, 4], P(('fsdp', 'rep')), may hold values from 1 to 128, 256 in all within a row
- seq_start: int32 [1024], P(('fsdp', 'rep')), may hold values from 0 to 2047
Outputs:
- input_grad: bfloat16 [262144, 2048], P(('fsdp', 'rep'))
- grad_update: float32 [2048, 768], P('fsdp')
- grad_norm: float32 [], replicated
The draws below stay inside these ranges and needn't reach their ends.
Inputs may be any that keep to these rules, and one draw needn't show every extreme that they name: `doc_lengths`: each row sums to 256; the longest document of each device has exactly 128 tokens.
All inputs are finite; a program needn't handle non-finite values.
Results may differ from the reference program's by a relative error of at most 0.014.
Values may be sent and summed in bfloat16 or wider, within the bound.
A program may use at most 64 MiB of HBM per device.

```python
import math
import jax
import jax.numpy as jnp
import numpy as np
from jax import lax

D = 2048
HEAD = 128
QH = 2
DOCS = 4
SEQ = 256
QW = 256
COLS = 768
TOKENS = 262144
N_FSDP = 16
N_REP = 64


def draw_hidden_in(key, part):
    base_key = jax.random.fold_in(key, 101)
    noise = jax.random.normal(jax.random.fold_in(base_key, 1), (TOKENS, D), jnp.float32)
    ramp = 0.4 * 3.0 ** (jnp.arange(D, dtype=jnp.float32) / (D - 1))
    return (noise * ramp[None, :]).astype(jnp.bfloat16)


def with_ends(drawn, stream_key, least, largest):
    longest = drawn.shape.index(max(drawn.shape))
    spots = []
    for shift in (0, 1):
        where = [jax.random.randint(jax.random.fold_in(stream_key, axis), (), 0, length) for axis, length in enumerate(drawn.shape)]
        where[longest] = (where[longest] + shift) % drawn.shape[longest]
        spots.append(tuple(where))
    return drawn.at[spots[0]].set(least).at[spots[1]].set(largest)


def steps_of(stream_key, extent, pieces, low, high):
    loudness, own = 1.0, jax.random.fold_in(stream_key, 6)
    for axis_at, parts in pieces:
        heights = jnp.exp(jax.random.uniform(jax.random.fold_in(own, axis_at), (parts,), jnp.float32, low / len(pieces), high / len(pieces)))
        loudness = loudness * jnp.repeat(heights, extent[axis_at] // parts).reshape([-1 if axis == axis_at else 1 for axis in range(len(extent))])
    return loudness


def length_profile(amount, total, reach, slope):
    loads = [(1 << 20) // math.isqrt(grade ** slope) + 1 for grade in range(2, amount + 1)]
    rest, counts = total - reach - (amount - 1), [1] * (amount - 1)
    while rest > 0:
        movable = [i for i in range(amount - 1) if counts[i] < reach]
        mass, budget = sum([loads[i] for i in movable]), rest
        for i in movable:
            more = min(reach - counts[i], max(1, budget * loads[i] // mass), rest)
            counts[i] = counts[i] + more
            rest = rest - more
    return np.array([reach] + counts)


def uneven_parts(rng, amount, total, bound, slope):
    if amount == 2:
        one = jax.random.randint(rng, (), max(1, total - bound), min(bound, total - 1) + 1)
        return jnp.stack([one, total - one])
    sizes = jnp.asarray(length_profile(amount, total, bound, slope), jnp.int32)
    couples = (amount - 1) // 2
    giver, sink = sizes[1:1 + 2 * couples:2], sizes[2:2 + 2 * couples:2]
    margin = jnp.minimum(giver - 1, bound - sink)
    moved = jax.random.randint(jax.random.fold_in(rng, 1), (couples,), 0, 1 << 20) % (margin + 1)
    sizes = sizes.at[1:1 + 2 * couples:2].set(giver - moved).at[2:2 + 2 * couples:2].set(sink + moved)
    return sizes[jax.random.permutation(jax.random.fold_in(rng, 2), amount)]


def centred(key, shape, scale, bound, cuts=(), kind=jnp.bfloat16):
    array = scale * jax.random.normal(key, shape, jnp.float32)
    if cuts:
        array = array * steps_of(key, shape, cuts, -0.22, 0.18)
    return jnp.clip(array, -bound, bound).astype(kind)


def setup_inputs(seed: int = 0) -> dict:
    key_list = jax.random.split(jax.random.key(seed), 9)
    return {
        "hidden_in": draw_hidden_in(jax.random.fold_in(key_list[8], 71), 0),
        "out_grad": centred(key_list[1], (TOKENS, D), 1.0, 6.0, ((0, 1024),)),
        "attn_saved": centred(key_list[2], (TOKENS, QW), 1.0, 6.0, ((0, 1024),)),
        "row_lse": jnp.clip(2.5 + 3.5 * jax.random.uniform(key_list[3], (TOKENS, QH), jnp.float32) ** steps_of(key_list[3], (TOKENS, QH), ((0, 1024),), -0.2, 0.2), 2.5, 6.0),
        "w_qkv": centred(key_list[4], (D, QW + 2 * HEAD), D ** -0.5, 0.125, ((0, 16),)),
        "w_out_t": centred(key_list[5], (D, QW), D ** -0.5, 0.125, ((0, 16),)),
        "doc_lengths": jax.vmap(lambda own: uneven_parts(own, DOCS, SEQ, SEQ // 2, 2))(jax.random.split(key_list[6], (N_FSDP * N_REP))).reshape((N_FSDP * N_REP, DOCS)).astype(jnp.int32),
        "seq_start": with_ends(jax.random.randint(key_list[7], (N_FSDP * N_REP,), 0, 8 * SEQ), jax.random.fold_in(key_list[7], 1), 0, (8 * SEQ) - 1).astype(jnp.int32),
    }


def rotary(values_in, positions, turn, head_size):
    rows = values_in.shape[0]
    heads_count = values_in.shape[1] // head_size
    half_size = head_size // 2
    inverse = 1000000.0 ** (-(jnp.arange(half_size, dtype=jnp.float32) * 2.0) / head_size)
    angles = positions.astype(jnp.float32)[:, None] * inverse[None, :]
    cosine = jnp.cos(angles)[:, None, :]
    sines = jnp.sin(angles)[:, None, :]
    shaped = values_in.reshape(rows, heads_count, head_size)
    first_half = shaped[:, :, :half_size]
    second_half = shaped[:, :, half_size:]
    result = jnp.concatenate([first_half * cosine - turn * second_half * sines, second_half * cosine + turn * first_half * sines], axis=2)
    return result.reshape(rows, heads_count * head_size)

def per_device(total, inputs):
    tokens_x, grads_y, saved, lse_rows, lengths, start, w_qkv, w_out_t = inputs
    scale = 1.0 / HEAD ** 0.5
    proj = jnp.dot(tokens_x, w_qkv, preferred_element_type=jnp.float32)
    attn_grad = jnp.dot(grads_y, w_out_t, preferred_element_type=jnp.float32).astype(jnp.bfloat16)
    positions = start + jnp.arange(SEQ, dtype=jnp.int32)
    queries = rotary(proj[:, :QW], positions, 1.0, HEAD).astype(jnp.bfloat16)
    keys = rotary(proj[:, QW:QW + HEAD], positions, 1.0, HEAD).astype(jnp.bfloat16)
    values_all = proj[:, QW + HEAD:].astype(jnp.bfloat16)
    ends = jnp.cumsum(lengths)
    local_rows = jnp.arange(SEQ, dtype=jnp.int32)
    documents = lax.optimization_barrier(jnp.sum((local_rows[:, None] >= ends[None, :]).astype(jnp.int32), axis=1))
    allowed = (documents[:, None] == documents[None, :]) & (local_rows[None, :] <= local_rows[:, None])
    key_grad = jnp.zeros((SEQ, HEAD), jnp.float32)
    value_grad = jnp.zeros((SEQ, HEAD), jnp.float32)
    query_parts = []
    for head_index in range(QH):
        lower = head_index * HEAD
        query_head = queries[:, lower:lower + HEAD]
        scores = jnp.dot(query_head, keys.T, preferred_element_type=jnp.float32) * scale
        probs = jnp.where(allowed, jnp.exp(scores - lse_rows[:, head_index:head_index + 1]), 0.0)
        grad_head = attn_grad[:, lower:lower + HEAD]
        dprobs = jnp.dot(grad_head, values_all.T, preferred_element_type=jnp.float32)
        delta = lax.optimization_barrier(jnp.sum(grad_head.astype(jnp.float32) * saved[:, lower:lower + HEAD].astype(jnp.float32), axis=1, keepdims=True))
        dscores = (probs * (dprobs - delta) * scale).astype(jnp.bfloat16)
        probs_low = probs.astype(jnp.bfloat16)
        value_grad = value_grad + jnp.dot(probs_low.T, grad_head, preferred_element_type=jnp.float32)
        query_parts.append(jnp.dot(dscores, keys, preferred_element_type=jnp.float32))
        key_grad = key_grad + jnp.dot(dscores.T, query_head, preferred_element_type=jnp.float32)
    query_grad = rotary(jnp.concatenate(query_parts, axis=1), positions, -1.0, HEAD).astype(jnp.bfloat16)
    key_grad = rotary(key_grad, positions, -1.0, HEAD).astype(jnp.bfloat16)
    d_qkv = jnp.concatenate([query_grad, key_grad, value_grad.astype(jnp.bfloat16)], axis=1)
    input_grad = jnp.dot(d_qkv, w_qkv.T, preferred_element_type=jnp.float32).astype(jnp.bfloat16)
    partial_term = jnp.concatenate([jnp.dot(tokens_x.T, d_qkv, preferred_element_type=jnp.float32), jnp.dot(grads_y.T, saved, preferred_element_type=jnp.float32)], axis=1)
    rounded = lax.optimization_barrier(partial_term.astype(jnp.bfloat16)).astype(jnp.float32)
    return (total + rounded, input_grad)

def reference(hidden_in, out_grad, attn_saved, row_lse, w_qkv, w_out_t, doc_lengths, seq_start):
    groups = doc_lengths.shape[0]

    def step_fn(total, inputs):
        return per_device(total, inputs + (w_qkv, w_out_t))
    stacked = (hidden_in.reshape(groups, SEQ, D), out_grad.reshape(groups, SEQ, D), attn_saved.reshape(groups, SEQ, QW), row_lse.reshape(groups, SEQ, QH), doc_lengths, seq_start)
    grads, input_grad = lax.scan(step_fn, jnp.zeros((D, COLS), jnp.float32), stacked)
    norm_sq = jnp.sum(grads * grads)
    grad_update = grads * lax.rsqrt(norm_sq / (D * COLS) + 1e-06)
    return (input_grad.reshape(TOKENS, D), grad_update, jnp.sqrt(norm_sq))
```

```python
import jax
import jax.numpy as jnp
import numpy as np
from jax import lax
from jax.experimental import pallas as pl
from jax.experimental.pallas import tpu as pltpu
from jax.sharding import Mesh
from jax.sharding import PartitionSpec as P

D = 2048
HEAD = 128
ROWS = 256
AXES = ("fsdp_0", "fsdp_1", "rep_0", "rep_1", "rep_2")
FSDP = AXES[:2]
FSDP_REP = AXES
F32 = jnp.float32
BF16 = jnp.bfloat16
SEMS = 360


def mod(value, size):
    return lax.rem(value + size, size)


def dot(left, right, contract=((1,), (0,))):
    return lax.dot_general(left, right, (contract, ((), ())), preferred_element_type=F32)


class Links:
    def __init__(self, sems):
        self.sems, self.used, self.started = sems, 0, []

    def send(self, src, dst, device):
        at = self.used
        self.used += 2
        copy = pltpu.make_async_remote_copy(
            src_ref=src,
            dst_ref=dst,
            send_sem=self.sems.at[at],
            recv_sem=self.sems.at[at + 1],
            device_id=device,
            device_id_type=pl.DeviceIdType.MESH,
        )
        copy.start()
        self.started.append(copy)
        return copy

    def finish(self):
        for copy in self.started:
            copy.wait_send()


def arrived(copies):
    for copy in copies:
        copy.wait_recv()


def kernel(
    start_ref,
    doc_ref,
    inv_ref,
    lse_ref,
    hid_hbm,
    og_hbm,
    as_hbm,
    wq_hbm,
    wo_hbm,
    ig_hbm,
    grads_ref,
    norm_ref,
    hid,
    og,
    saved,
    wbuf,
    hid_t,
    og_t,
    proj,
    cos_ref,
    sin_ref,
    dqkv,
    igv,
    gs_y,
    gs_x,
    gs_z,
    gr_y,
    gr_x,
    gr_z,
    s_y,
    s_x,
    s_z,
    r_y,
    r_x,
    r_z,
    s2_y,
    s2_x,
    s2_z,
    r2_y,
    r2_x,
    r2_z,
    r3_y,
    s3_x,
    r3_x,
    r3_z,
    fa,
    fx,
    nz,
    ny,
    sems,
    local,
):
    y = lax.axis_index(AXES[0])
    zh = lax.axis_index(AXES[1])
    zl = lax.axis_index(AXES[2])
    x = lax.axis_index(AXES[3])
    c = lax.axis_index(AXES[4])
    z = zh * 4 + zl
    mate = (y, zh, zl, x, 1 - c)
    mirror = (y, 1 - zh, 3 - zl, x, c)

    def at_y(d):
        return (mod(y + d, 8), zh, zl, x, c)

    def at_x(d, dc=0):
        return (y, zh, zl, mod(x + d, 8), mod(c + dc, 2))

    def at_z(d):
        there = mod(z + d, 8)
        return (y, there // 4, lax.rem(there, 4), x, c)

    def at_zl(d, dc):
        return (y, zh, mod(zl + d, 4), x, mod(c + dc, 2))

    peers = [mate]
    peers += [at_y(d) for d in range(1, 8)]
    peers += [at_x(d, dc) for d in range(1, 8) for dc in range(2)]
    peers += [at_z(d) for d in range(1, 8)]
    peers += [at_zl(d, 1) for d in range(1, 4)]
    barrier = pltpu.get_barrier_semaphore()
    extra = len(peers)
    for peer in peers:
        pl.semaphore_signal(barrier, inc=1, device_id=peer, device_id_type=pl.DeviceIdType.MESH)

    def rows_of(block, first, count):
        return pl.ds(pl.multiple_of(block * 128 + first, 32), count)

    own = y * 2 + zh
    own_rows = rows_of(own, 0, 128)
    load_wq = pltpu.make_async_copy(wq_hbm, wbuf.at[own_rows, pl.ds(0, 512)], local.at[0])
    load_wo = pltpu.make_async_copy(wo_hbm, wbuf.at[own_rows, pl.ds(512, 256)], local.at[1])
    load_og = pltpu.make_async_copy(og_hbm, og, local.at[2])
    load_as = pltpu.make_async_copy(as_hbm, saved, local.at[3])
    load_hid = pltpu.make_async_copy(hid_hbm, hid, local.at[4])
    for copy in (load_wq, load_wo, load_og, load_as, load_hid):
        copy.start()
    load_wq.wait()
    load_wo.wait()
    pl.semaphore_wait(barrier, extra)

    links = Links(sems)

    def weight(block, first, count, device):
        ref = wbuf.at[rows_of(block, first, count), :]
        return links.send(ref, ref, device)

    half = c * 64
    other_half = 1 - zh
    to_mirror = weight(own, half, 64, mirror)
    up, down = at_y(1), at_y(-1)
    shared = []

    class Ring:
        def __init__(self, zside):
            self.zside = zside
            self.sent = [self.pass_on(0)]

        def block(self, d):
            return mod(y + d, 8) * 2 + self.zside

        def pass_on(self, s):
            if s < 3:
                return (
                    weight(self.block(-s), half, 64, up),
                    weight(self.block(s), half, 64, down),
                )
            return (
                weight(self.block(-3), half, 32, up),
                weight(self.block(3), half + 32, 32, down),
            )

        def step(self, s):
            arrived(self.sent[-1])
            if s < 4:
                self.sent.append(self.pass_on(s))
                shared.append(weight(self.block(-s), half, 64, mate))
                shared.append(weight(self.block(s), half, 64, mate))
            else:
                shared.append(weight(self.block(4), half, 64, mate))

    ring_a = Ring(zh)

    positions = (start_ref[0] + lax.broadcasted_iota(jnp.int32, (ROWS, HEAD), 0)).astype(F32)
    angles = positions * inv_ref[...]
    sign = jnp.where(lax.broadcasted_iota(jnp.int32, (ROWS, HEAD), 1) < HEAD // 2, -1.0, 1.0)
    cos_ref[...] = jnp.cos(angles)
    sin_ref[...] = jnp.sin(angles) * sign

    def transpose(src, dst, j):
        part = src[:, 256 * j : 256 * (j + 1)].T
        for i in range(2):
            for h in range(2):
                b = 2 * j + i
                dst[h, b * 64 : (b + 1) * 64, :] = part[i * 128 + h * 64 : i * 128 + h * 64 + 64]

    to_mirror.wait_recv()
    ring_b = Ring(other_half)
    shared.append(weight(y * 2 + other_half, half, 64, mate))
    load_og.wait()
    load_as.wait()
    for j in range(4):
        transpose(og, og_t, j)
    ring_a.step(1)
    for j in range(4, 8):
        transpose(og, og_t, j)

    def put_z(dst, block, tile):
        for qr in range(4):
            zz = (block % 2) * 4 + qr
            yy = block // 2
            dst[zz, yy * 16 : yy * 16 + 16, :] = tile[qr * 16 : qr * 16 + 16]

    def out_term(h, ch):
        return dot(og_t[h, ch * 256 : (ch + 1) * 256, :], saved[...])

    for ch in range(4):
        part = out_term(1 - c, ch).astype(BF16)
        for i in range(4):
            put_z(gs_z, ch * 4 + i, part[i * 64 : i * 64 + 64])
    core_z = links.send(gs_z, gr_z, mate)
    ring_b.step(1)
    ring_a.step(2)
    for ch in range(4):
        part = out_term(c, ch)
        for i in range(4):
            put_z(s_z, ch * 4 + i, part[i * 64 : i * 64 + 64].astype(BF16))
    core_z.wait_recv()
    for k in range(8):
        s_z[k] = (s_z[k].astype(F32) + gr_z[k].astype(F32)).astype(BF16)
    first_z = [links.send(s_z.at[mod(z + d, 8)], r_z.at[d - 1], at_z(d)) for d in range(1, 8)]
    ring_b.step(2)
    load_hid.wait()
    for j in range(4):
        transpose(hid, hid_t, j)
    ring_a.step(3)
    for j in range(4, 8):
        transpose(hid, hid_t, j)
    ring_b.step(3)
    ring_a.step(4)
    ring_b.step(4)
    arrived(shared)

    proj[:, :512] = dot(hid[...], wbuf[:, :512])
    proj[:, 512:] = dot(og[...], wbuf[:, 512:])
    cosine, sines = cos_ref[...], sin_ref[...]

    def rotary(value):
        return value * cosine + pltpu.roll(value, HEAD // 2, 1) * sines

    def rotary_back(value):
        return value * cosine - pltpu.roll(value, HEAD // 2, 1) * sines

    keys = rotary(proj[:, 256:384]).astype(BF16)
    values = proj[:, 384:512].astype(BF16)
    row = lax.broadcasted_iota(jnp.int32, (ROWS, ROWS), 0)
    col = lax.broadcasted_iota(jnp.int32, (ROWS, ROWS), 1)
    allowed = col <= row
    end = jnp.int32(0)
    for i in range(4):
        end = end + doc_ref[0, i]
        allowed = allowed & ((row >= end) == (col >= end))
    scale = 1.0 / HEAD**0.5
    key_grad = jnp.zeros((ROWS, HEAD), F32)
    value_grad = jnp.zeros((ROWS, HEAD), F32)
    for h in range(2):
        lanes = slice(h * HEAD, (h + 1) * HEAD)
        query = rotary(proj[:, lanes]).astype(BF16)
        grad = proj[:, 512 + h * HEAD : 512 + (h + 1) * HEAD].astype(BF16)
        scores = dot(query, keys, ((1,), (1,))) * scale
        probs = jnp.where(allowed, jnp.exp(scores - lse_ref[:, h : h + 1]), 0.0)
        dprobs = dot(grad, values, ((1,), (1,)))
        delta = jnp.sum(
            grad.astype(F32) * saved[:, lanes].astype(F32), axis=1, keepdims=True
        )
        dscores = (probs * (dprobs - delta) * scale).astype(BF16)
        value_grad += dot(probs.astype(BF16), grad, ((0,), (0,)))
        key_grad += dot(dscores, query, ((0,), (0,)))
        dqkv[:, lanes] = rotary_back(dot(dscores, keys)).astype(BF16)
    dqkv[:, 256:384] = rotary_back(key_grad).astype(BF16)
    dqkv[:, 384:512] = value_grad.astype(BF16)

    def put_yx(dst_y, dst_x, block, tile):
        yy, side = block // 2, block % 2
        dst_y[yy, side * 64 : side * 64 + 64, :] = tile[:, :256]
        for qr in range(4):
            for ct in range(2):
                dst_x[qr * 2 + ct, block * 16 : block * 16 + 16, :] = tile[
                    qr * 16 : qr * 16 + 16, 256 + ct * 128 : 384 + ct * 128
                ]

    def qkv_term(h, ch):
        return dot(hid_t[h, ch * 256 : (ch + 1) * 256, :], dqkv[...])

    core_y, core_x = [], []
    for ch in range(4):
        part = qkv_term(1 - c, ch).astype(BF16)
        for i in range(4):
            put_yx(gs_y, gs_x, ch * 4 + i, part[i * 64 : i * 64 + 64])
        where = pl.ds(ch * 2, 2)
        core_y.append(links.send(gs_y.at[where], gr_y.at[where], mate))
        where = (slice(None), pl.ds(ch * 64, 64), slice(None))
        core_x.append(links.send(gs_x.at[where], gr_x.at[where], mate))
    for ch in range(4):
        part = qkv_term(c, ch).astype(BF16)
        for i in range(4):
            put_yx(s_y, s_x, ch * 4 + i, part[i * 64 : i * 64 + 64])
    arrived(core_y)
    for k in range(8):
        s_y[k] = (s_y[k].astype(F32) + gr_y[k].astype(F32)).astype(BF16)
    first_y = [links.send(s_y.at[mod(y + d, 8)], r_y.at[d - 1], at_y(d)) for d in range(1, 8)]
    arrived(core_x)
    for k in range(8):
        s_x[k] = (s_x[k].astype(F32) + gr_x[k].astype(F32)).astype(BF16)
    first_x = [links.send(s_x.at[mod(x + d, 8)], r_x.at[d - 1], at_x(d)) for d in range(1, 8)]

    def summed(own_part, parts):
        total = own_part.astype(F32)
        for i in range(7):
            total = total + parts[i].astype(F32)
        return total

    def in_order(parts):
        total = parts[0].astype(F32)
        for i in range(1, 8):
            total = total + parts[i].astype(F32)
        return total

    arrived(first_z)
    total = summed(s_z[z], r_z).astype(BF16)
    for k in range(8):
        s2_z[k] = total[k * 16 : k * 16 + 16]
    second_z = [links.send(s2_z.at[mod(y + d, 8)], r2_z.at[d - 1], at_y(d)) for d in range(1, 8)]

    for n in range(4):
        cols = slice(n * 512, (n + 1) * 512)
        igv[:, cols] = dot(dqkv[...], wbuf[cols, :512], ((1,), (1,))).astype(BF16)
    store_ig = pltpu.make_async_copy(igv, ig_hbm, local.at[5])
    store_ig.start()

    arrived(second_z)
    r3_z[x] = summed(s2_z[y], r2_z).astype(BF16)
    third_z = [links.send(r3_z.at[x], r3_z.at[x], at_x(d)) for d in range(1, 8)]

    arrived(first_y)
    total = summed(s_y[y], r_y).astype(BF16)
    for k in range(8):
        s2_y[k] = total[k * 16 : k * 16 + 16]
    second_y = [links.send(s2_y.at[mod(z + d, 8)], r2_y.at[d - 1], at_z(d)) for d in range(1, 8)]
    arrived(first_x)
    total = summed(s_x[x], r_x).astype(BF16)
    for k in range(8):
        s2_x[k] = total[k * 32 : k * 32 + 32]
    second_x = [links.send(s2_x.at[mod(y + d, 8)], r2_x.at[d - 1], at_y(d)) for d in range(1, 8)]

    mine = c * 4 + zl
    arrived(third_z)
    fa[mine, :, 256:512] = in_order(r3_z)

    arrived(second_y)
    r3_y[x] = summed(s2_y[z], r2_y).astype(BF16)
    third_y = [links.send(r3_y.at[x], r3_y.at[x], at_x(d)) for d in range(1, 8)]
    arrived(second_x)
    total = summed(s2_x[y], r2_x).astype(BF16)
    for k in range(2):
        s3_x[k] = total[k * 16 : k * 16 + 16]
    r3_x[z] = s3_x[zh]
    third_x = [
        links.send(s3_x.at[mod(z + d, 8) // 4], r3_x.at[z], at_z(d)) for d in range(1, 8)
    ]

    arrived(third_y)
    fa[mine, :, 0:256] = in_order(r3_y)
    spread = [
        links.send(fa.at[mine], fa.at[mine], at_zl(d, dc) if d else mate)
        for d in range(4)
        for dc in range(2)
        if d or dc
    ]
    arrived(third_x)
    tile = c * 8 + x
    fx[tile] = in_order(r3_x)
    spread += [
        links.send(fx.at[tile], fx.at[tile], at_x(d, dc) if d else mate)
        for d in range(8)
        for dc in range(2)
        if d or dc
    ]
    arrived(spread)
    for i in range(8):
        grads_ref[i * 16 : i * 16 + 16, 0:256] = fa[i, :, 0:256]
        grads_ref[i * 16 : i * 16 + 16, 512:768] = fa[i, :, 256:512]
        for ct in range(2):
            at = (i // 4) * 8 + (i % 4) * 2 + ct
            grads_ref[i * 16 : i * 16 + 16, 256 + ct * 128 : 384 + ct * 128] = fx[at]
    whole = grads_ref[...]
    square = (whole * whole).reshape(16, 8, 768).sum(axis=0)
    tile_sum = square[:, 0:128]
    for i in range(1, 6):
        tile_sum = tile_sum + square[:, i * 128 : i * 128 + 128]
    nz[0] = tile_sum
    across = links.send(nz.at[0], nz.at[1], mirror)
    across.wait_recv()
    ny[y] = nz[0] + nz[1]
    along = [links.send(ny.at[y], ny.at[y], at_y(d)) for d in range(1, 8)]
    arrived(along)
    total = ny[0]
    for i in range(1, 8):
        total = total + ny[i]
    norm_ref[...] = total
    links.finish()
    store_ig.wait()
    assert links.used <= SEMS


def body(hidden_in, out_grad, attn_saved, row_lse, w_qkv, w_out_t, doc_lengths, seq_start):
    power = np.arange(HEAD // 2, dtype=np.float64) * 2.0 / HEAD
    inverse = np.tile(1000000.0 ** (-power), 2).astype(np.float32)[None, :]
    smem = pl.BlockSpec(memory_space=pltpu.SMEM)
    vmem = pl.BlockSpec(memory_space=pltpu.VMEM)
    hbm = pl.BlockSpec(memory_space=pl.ANY)
    half = (8, 128, 256)
    tall = (8, 256, 128)

    def bf(*shape):
        return pltpu.VMEM(shape, BF16)

    def f32(*shape):
        return pltpu.VMEM(shape, F32)

    input_grad, grads, tiles = pl.pallas_call(
        kernel,
        out_shape=(
            jax.ShapeDtypeStruct((ROWS, D), BF16),
            jax.ShapeDtypeStruct((128, 768), F32),
            jax.ShapeDtypeStruct((8, 128), F32),
        ),
        in_specs=[smem, smem, vmem, vmem, hbm, hbm, hbm, hbm, hbm],
        out_specs=(hbm, vmem, vmem),
        scratch_shapes=[
            bf(ROWS, D),
            bf(ROWS, D),
            bf(ROWS, 256),
            bf(D, 768),
            bf(2, 1024, 256),
            bf(2, 1024, 256),
            f32(ROWS, 768),
            f32(ROWS, HEAD),
            f32(ROWS, HEAD),
            bf(ROWS, 512),
            bf(ROWS, D),
            bf(*half),
            bf(*tall),
            bf(*half),
            bf(*half),
            bf(*tall),
            bf(*half),
            bf(*half),
            bf(*tall),
            bf(*half),
            bf(7, 128, 256),
            bf(7, 256, 128),
            bf(7, 128, 256),
            bf(8, 16, 256),
            bf(8, 32, 128),
            bf(8, 16, 256),
            bf(7, 16, 256),
            bf(7, 32, 128),
            bf(7, 16, 256),
            bf(8, 16, 256),
            bf(2, 16, 128),
            bf(8, 16, 128),
            bf(8, 16, 256),
            f32(8, 16, 512),
            f32(16, 16, 128),
            f32(2, 8, 128),
            f32(8, 8, 128),
            pltpu.SemaphoreType.DMA((SEMS,)),
            pltpu.SemaphoreType.DMA((6,)),
        ],
        compiler_params=pltpu.CompilerParams(collective_id=0, has_side_effects=True),
        name="attention_backward",
    )(
        seq_start,
        doc_lengths,
        jnp.asarray(inverse),
        row_lse,
        hidden_in,
        out_grad,
        attn_saved,
        w_qkv,
        w_out_t,
    )
    norm_sq = jnp.sum(tiles)
    grad_update = grads * lax.rsqrt(norm_sq / (D * 768) + 1e-06)
    return (input_grad, grad_update, jnp.sqrt(norm_sq))


def solution(mesh):
    split = Mesh(mesh.devices.reshape(8, 2, 4, 8, 2), AXES)
    tokens = P(FSDP_REP, None)
    in_specs = (tokens, tokens, tokens, tokens, P(FSDP, None), P(FSDP, None), tokens, P(FSDP_REP))
    out_specs = (tokens, P(FSDP, None), P())
    return jax.shard_map(body, mesh=split, in_specs=in_specs, out_specs=out_specs, check_vma=False)
```

```python
import jax
import jax.numpy as jnp
import numpy as np
from jax import lax
from jax.experimental import pallas as pl
from jax.experimental.pallas import tpu as pltpu
from jax.sharding import Mesh
from jax.sharding import PartitionSpec as P

D = 2048
HEAD = 128
ROWS = 256
AXES = ("fsdp_0", "fsdp_1", "rep_0", "rep_1", "rep_2")
FSDP = AXES[:2]
FSDP_REP = AXES
F32 = jnp.float32
BF16 = jnp.bfloat16
SEMS = 360


def mod(value, size):
    return lax.rem(value + size, size)


def dot(left, right, contract=((1,), (0,))):
    return lax.dot_general(left, right, (contract, ((), ())), preferred_element_type=F32)


class Links:
    def __init__(self, sems):
        self.sems, self.used, self.started = sems, 0, []

    def send(self, src, dst, device):
        at = self.used
        self.used += 2
        copy = pltpu.make_async_remote_copy(
            src_ref=src,
            dst_ref=dst,
            send_sem=self.sems.at[at],
            recv_sem=self.sems.at[at + 1],
            device_id=device,
            device_id_type=pl.DeviceIdType.MESH,
        )
        copy.start()
        self.started.append(copy)
        return copy

    def finish(self):
        for copy in self.started:
            copy.wait_send()


def arrived(copies):
    for copy in copies:
        copy.wait_recv()


def kernel(
    start_ref,
    doc_ref,
    inv_ref,
    lse_ref,
    hid_hbm,
    og_hbm,
    as_hbm,
    wq_hbm,
    wo_hbm,
    ig_ref,
    grads_ref,
    norm_ref,
    hid,
    og,
    saved,
    wbuf,
    hid_t,
    og_t,
    proj,
    lse,
    cos_ref,
    sin_ref,
    dqkv,
    gs_y,
    gs_x,
    gs_z,
    gr_y,
    gr_x,
    gr_z,
    s_y,
    s_x,
    s_z,
    r_y,
    r_x,
    r_z,
    s2_y,
    s2_x,
    s2_z,
    r2_y,
    r2_x,
    r2_z,
    r3_y,
    s3_x,
    r3_x,
    r3_z,
    far_y,
    far_x,
    far_z,
    fy,
    fz,
    fx,
    ny,
    sems,
    local,
):
    y = lax.axis_index(AXES[0])
    zh = lax.axis_index(AXES[1])
    zl = lax.axis_index(AXES[2])
    x = lax.axis_index(AXES[3])
    c = lax.axis_index(AXES[4])
    z = zh * 4 + zl
    mate = (y, zh, zl, x, 1 - c)
    mirror = (y, 1 - zh, 3 - zl, x, c)

    def at_y(d):
        return (mod(y + d, 8), zh, zl, x, c)

    def at_x(d, dc=0):
        return (y, zh, zl, mod(x + d, 8), mod(c + dc, 2))

    def at_z(d):
        there = mod(z + d, 8)
        return (y, there // 4, lax.rem(there, 4), x, c)

    def across(d):
        return (mod(y + d, 8), 1 - zh, 3 - zl, x, c)

    def at_zl(d, dc):
        return (y, zh, mod(zl + d, 4), x, mod(c + dc, 2))

    peers = [mate]
    peers += [at_y(d) for d in range(1, 8)]
    peers += [at_x(d, dc) for d in range(1, 8) for dc in range(2)]
    peers += [at_z(d) for d in range(1, 8)]
    peers += [at_zl(d, 1) for d in range(1, 4)]
    peers += [across(d) for d in range(1, 8)]
    barrier = pltpu.get_barrier_semaphore()
    extra = len(peers)
    for peer in peers:
        pl.semaphore_signal(barrier, inc=1, device_id=peer, device_id_type=pl.DeviceIdType.MESH)

    def rows_of(block, first, count):
        return pl.ds(pl.multiple_of(block * 128 + first, 32), count)

    own = y * 2 + zh
    own_rows = rows_of(own, 0, 128)
    load_wq = pltpu.make_async_copy(wq_hbm, wbuf.at[own_rows, pl.ds(0, 512)], local.at[0])
    load_wo = pltpu.make_async_copy(wo_hbm, wbuf.at[own_rows, pl.ds(512, 256)], local.at[1])
    load_og = pltpu.make_async_copy(og_hbm, og, local.at[2])
    load_as = pltpu.make_async_copy(as_hbm, saved, local.at[3])
    load_hid = pltpu.make_async_copy(hid_hbm, hid, local.at[4])
    for copy in (load_wq, load_wo, load_og, load_as, load_hid):
        copy.start()
    load_wq.wait()
    load_wo.wait()
    pl.semaphore_wait(barrier, extra)

    links = Links(sems)

    def weight(block, first, count, device):
        ref = wbuf.at[rows_of(block, first, count), :]
        return links.send(ref, ref, device)

    half = c * 64
    other_half = 1 - zh
    to_mirror = weight(own, half, 64, mirror)
    up, down = at_y(1), at_y(-1)
    shared = []

    class Ring:
        def __init__(self, zside):
            self.zside = zside
            self.sent = [self.pass_on(0)]

        def block(self, d):
            return mod(y + d, 8) * 2 + self.zside

        def pass_on(self, s):
            if s < 3:
                return (
                    weight(self.block(-s), half, 64, up),
                    weight(self.block(s), half, 64, down),
                )
            return (
                weight(self.block(-3), half, 32, up),
                weight(self.block(3), half + 32, 32, down),
            )

        def step(self, s):
            arrived(self.sent[-1])
            if s < 4:
                self.sent.append(self.pass_on(s))
                shared.append(weight(self.block(-s), half, 64, mate))
                shared.append(weight(self.block(s), half, 64, mate))
            else:
                shared.append(weight(self.block(4), half, 64, mate))

    ring_a = Ring(zh)

    positions = (start_ref[0] + lax.broadcasted_iota(jnp.int32, (ROWS, HEAD), 0)).astype(F32)
    angles = positions * inv_ref[...]
    sign = jnp.where(lax.broadcasted_iota(jnp.int32, (ROWS, HEAD), 1) < HEAD // 2, -1.0, 1.0)
    for h in range(2):
        lse[h] = jnp.broadcast_to(lse_ref[h : h + 1, :], (HEAD, ROWS)).T
    cos_ref[...] = jnp.cos(angles)
    sin_ref[...] = jnp.sin(angles) * sign

    def transpose(src, dst, j):
        part = src[:, 256 * j : 256 * (j + 1)].T
        for i in range(2):
            for h in range(2):
                b = 2 * j + i
                dst[h, b * 64 : (b + 1) * 64, :] = part[i * 128 + h * 64 : i * 128 + h * 64 + 64]

    to_mirror.wait_recv()
    ring_b = Ring(other_half)
    shared.append(weight(y * 2 + other_half, half, 64, mate))
    load_og.wait()
    load_as.wait()
    for j in range(4):
        transpose(og, og_t, j)
    ring_a.step(1)
    for j in range(4, 8):
        transpose(og, og_t, j)

    sign_c = 1 - 2 * c

    class First:
        def __init__(self, chunks, parts, relay, me, at):
            self.chunks, self.parts, self.relay, self.me, self.at = chunks, parts, relay, me, at
            self.far = links.send(chunks.at[mod(me + 4, 8)], relay, at(sign_c))
            self.sent = [self.go(i, d) for i, d in enumerate((-3, 2, -2, 1, -1))]

        def go(self, i, d):
            there = mod(self.me + sign_c * d, 8)
            return links.send(self.chunks.at[there], self.parts.at[i], self.at(sign_c * d))

        def pass_on(self):
            self.far.wait_recv()
            there = mod(self.me + sign_c * 3, 8)
            both = self.chunks[there].astype(F32) + self.relay[...].astype(F32)
            self.chunks[there] = both.astype(BF16)
            self.sent.append(self.go(5, 3))

        def total(self):
            arrived(self.sent)
            return summed(self.chunks[self.me], self.parts, 6).astype(BF16)

    def summed(own_part, parts, count):
        total = own_part.astype(F32)
        for i in range(count):
            total = total + parts[i].astype(F32)
        return total

    def in_order(parts):
        total = parts[0].astype(F32)
        for i in range(1, 8):
            total = total + parts[i].astype(F32)
        return total

    def put_z(dst, block, tile):
        for qr in range(4):
            zz = (block % 2) * 4 + qr
            yy = block // 2
            dst[zz, yy * 16 : yy * 16 + 16, :] = tile[qr * 16 : qr * 16 + 16]

    def out_term(h, ch):
        return dot(og_t[h, ch * 256 : (ch + 1) * 256, :], saved[...])

    for ch in range(4):
        part = out_term(1 - c, ch).astype(BF16)
        for i in range(4):
            put_z(gs_z, ch * 4 + i, part[i * 64 : i * 64 + 64])
    core_z = links.send(gs_z, gr_z, mate)
    ring_b.step(1)
    ring_a.step(2)
    for ch in range(4):
        part = out_term(c, ch)
        for i in range(4):
            put_z(s_z, ch * 4 + i, part[i * 64 : i * 64 + 64].astype(BF16))
    core_z.wait_recv()
    for k in range(8):
        s_z[k] = (s_z[k].astype(F32) + gr_z[k].astype(F32)).astype(BF16)
    first_z = First(s_z, r_z, far_z, z, at_z)
    ring_b.step(2)
    first_z.pass_on()
    load_hid.wait()
    for j in range(4):
        transpose(hid, hid_t, j)
    ring_a.step(3)
    for j in range(4, 8):
        transpose(hid, hid_t, j)
    ring_b.step(3)
    ring_a.step(4)
    ring_b.step(4)
    arrived(shared)

    proj[:, :512] = dot(hid[...], wbuf[:, :512])
    proj[:, 512:] = dot(og[...], wbuf[:, 512:])
    cosine, sines = cos_ref[...], sin_ref[...]

    def rotary(value):
        return value * cosine + pltpu.roll(value, HEAD // 2, 1) * sines

    def rotary_back(value):
        return value * cosine - pltpu.roll(value, HEAD // 2, 1) * sines

    keys = rotary(proj[:, 256:384]).astype(BF16)
    values = proj[:, 384:512].astype(BF16)
    row = lax.broadcasted_iota(jnp.int32, (ROWS, ROWS), 0)
    col = lax.broadcasted_iota(jnp.int32, (ROWS, ROWS), 1)
    allowed = col <= row
    end = jnp.int32(0)
    for i in range(4):
        end = end + doc_ref[0, i]
        allowed = allowed & ((row >= end) == (col >= end))
    scale = 1.0 / HEAD**0.5
    key_grad = jnp.zeros((ROWS, HEAD), F32)
    value_grad = jnp.zeros((ROWS, HEAD), F32)
    for h in range(2):
        lanes = slice(h * HEAD, (h + 1) * HEAD)
        query = rotary(proj[:, lanes]).astype(BF16)
        grad = proj[:, 512 + h * HEAD : 512 + (h + 1) * HEAD].astype(BF16)
        scores = dot(query, keys, ((1,), (1,))) * scale
        probs = jnp.where(allowed, jnp.exp(scores - lse[h, :, 0:1]), 0.0)
        dprobs = dot(grad, values, ((1,), (1,)))
        delta = jnp.sum(
            grad.astype(F32) * saved[:, lanes].astype(F32), axis=1, keepdims=True
        )
        dscores = (probs * (dprobs - delta) * scale).astype(BF16)
        value_grad += dot(probs.astype(BF16), grad, ((0,), (0,)))
        key_grad += dot(dscores, query, ((0,), (0,)))
        dqkv[:, lanes] = rotary_back(dot(dscores, keys)).astype(BF16)
    dqkv[:, 256:384] = rotary_back(key_grad).astype(BF16)
    dqkv[:, 384:512] = value_grad.astype(BF16)

    def put_yx(dst_y, dst_x, block, tile):
        yy, side = block // 2, block % 2
        dst_y[yy, side * 64 : side * 64 + 64, :] = tile[:, :256]
        for qr in range(4):
            for ct in range(2):
                dst_x[qr * 2 + ct, block * 16 : block * 16 + 16, :] = tile[
                    qr * 16 : qr * 16 + 16, 256 + ct * 128 : 384 + ct * 128
                ]

    def qkv_term(h, ch):
        return dot(hid_t[h, ch * 256 : (ch + 1) * 256, :], dqkv[...])

    core_y, core_x = [], []
    for ch in range(4):
        part = qkv_term(1 - c, ch).astype(BF16)
        for i in range(4):
            put_yx(gs_y, gs_x, ch * 4 + i, part[i * 64 : i * 64 + 64])
        where = pl.ds(ch * 2, 2)
        core_y.append(links.send(gs_y.at[where], gr_y.at[where], mate))
        where = (slice(None), pl.ds(ch * 64, 64), slice(None))
        core_x.append(links.send(gs_x.at[where], gr_x.at[where], mate))
    for ch in range(4):
        part = qkv_term(c, ch).astype(BF16)
        for i in range(4):
            put_yx(s_y, s_x, ch * 4 + i, part[i * 64 : i * 64 + 64])
    total = first_z.total()
    for k in range(8):
        s2_z[k] = total[k * 16 : k * 16 + 16]
    second_z = [links.send(s2_z.at[mod(y + d, 8)], r2_z.at[d - 1], at_y(d)) for d in range(1, 8)]
    arrived(core_y)
    for k in range(8):
        s_y[k] = (s_y[k].astype(F32) + gr_y[k].astype(F32)).astype(BF16)
    first_y = First(s_y, r_y, far_y, y, at_y)
    arrived(core_x)
    for k in range(8):
        s_x[k] = (s_x[k].astype(F32) + gr_x[k].astype(F32)).astype(BF16)
    first_x = First(s_x, r_x, far_x, x, at_x)

    for n in range(4):
        cols = slice(n * 512, (n + 1) * 512)
        ig_ref[:, cols] = dot(dqkv[...], wbuf[cols, :512], ((1,), (1,))).astype(BF16)
    first_y.pass_on()
    first_x.pass_on()

    arrived(second_z)
    r3_z[x] = summed(s2_z[y], r2_z, 7).astype(BF16)
    third_z = [links.send(r3_z.at[x], r3_z.at[x], at_x(d)) for d in range(1, 8)]

    total = first_y.total()
    for k in range(8):
        s2_y[k] = total[k * 16 : k * 16 + 16]
    second_y = [links.send(s2_y.at[mod(z + d, 8)], r2_y.at[d - 1], at_z(d)) for d in range(1, 8)]
    total = first_x.total()
    for k in range(8):
        s2_x[k] = total[k * 32 : k * 32 + 32]
    second_x = [links.send(s2_x.at[mod(y + d, 8)], r2_x.at[d - 1], at_y(d)) for d in range(1, 8)]

    def spread_zl(pieces):
        return [
            links.send(pieces.at[mine], pieces.at[mine], at_zl(d, dc) if d else mate)
            for d in range(4)
            for dc in range(2)
            if d or dc
        ]

    mine = c * 4 + zl
    arrived(third_z)
    fz[mine] = in_order(r3_z).astype(BF16)
    spread = spread_zl(fz)

    arrived(second_y)
    r3_y[x] = summed(s2_y[z], r2_y, 7).astype(BF16)
    third_y = [links.send(r3_y.at[x], r3_y.at[x], at_x(d)) for d in range(1, 8)]
    arrived(second_x)
    total = summed(s2_x[y], r2_x, 7).astype(BF16)
    for k in range(2):
        s3_x[k] = total[k * 16 : k * 16 + 16]
    r3_x[z] = s3_x[zh]
    third_x = [
        links.send(s3_x.at[mod(z + d, 8) // 4], r3_x.at[z], at_z(d)) for d in range(1, 8)
    ]

    arrived(third_y)
    fy[mine] = in_order(r3_y).astype(BF16)
    spread += spread_zl(fy)
    arrived(third_x)
    tile = c * 8 + x
    fx[tile] = in_order(r3_x).astype(BF16)
    spread += [
        links.send(fx.at[tile], fx.at[tile], at_x(d, dc) if d else mate)
        for d in range(8)
        for dc in range(2)
        if d or dc
    ]
    arrived(spread)
    for i in range(8):
        grads_ref[i * 16 : i * 16 + 16, 0:256] = fy[i].astype(F32)
        grads_ref[i * 16 : i * 16 + 16, 512:768] = fz[i].astype(F32)
        for ct in range(2):
            at = (i // 4) * 8 + (i % 4) * 2 + ct
            grads_ref[i * 16 : i * 16 + 16, 256 + ct * 128 : 384 + ct * 128] = fx[at].astype(F32)
    whole = grads_ref[...]
    square = (whole * whole).reshape(16, 8, 768).sum(axis=0)
    tile_sum = square[:, 0:128]
    for i in range(1, 6):
        tile_sum = tile_sum + square[:, i * 128 : i * 128 + 128]
    ny[own] = tile_sum
    along = [links.send(ny.at[own], ny.at[own], at_y(d)) for d in range(1, 8)]
    along += [links.send(ny.at[own], ny.at[own], across(d)) for d in range(8)]
    arrived(along)
    total = ny[0]
    for i in range(1, 16):
        total = total + ny[i]
    norm_ref[...] = total
    links.finish()
    assert links.used <= SEMS


def finish(ig_ref, grads_ref, tiles_ref, ig_out, update_ref, norm_ref, sem):
    store = pltpu.make_async_copy(ig_ref, ig_out, sem)
    store.start()
    norm_sq = jnp.sum(jnp.sum(tiles_ref[...], axis=0, keepdims=True), axis=1, keepdims=True)
    update_ref[...] = grads_ref[...] * lax.rsqrt(norm_sq / (D * 768) + 1e-06)
    norm_ref[...] = jnp.sqrt(norm_sq)
    store.wait()


def body(hidden_in, out_grad, attn_saved, row_lse, w_qkv, w_out_t, doc_lengths, seq_start):
    power = np.arange(HEAD // 2, dtype=np.float64) * 2.0 / HEAD
    inverse = np.tile(1000000.0 ** (-power), 2).astype(np.float32)[None, :]
    smem = pl.BlockSpec(memory_space=pltpu.SMEM)
    vmem = pl.BlockSpec(memory_space=pltpu.VMEM)
    hbm = pl.BlockSpec(memory_space=pl.ANY)
    half = (8, 128, 256)
    tall = (8, 256, 128)

    def bf(*shape):
        return pltpu.VMEM(shape, BF16)

    def f32(*shape):
        return pltpu.VMEM(shape, F32)

    input_grad, grads, tiles = pl.pallas_call(
        kernel,
        out_shape=(bf(ROWS, D), f32(128, 768), f32(8, 128)),
        in_specs=[smem, smem, vmem, vmem, hbm, hbm, hbm, hbm, hbm],
        out_specs=(vmem, vmem, vmem),
        scratch_shapes=[
            bf(ROWS, D),
            bf(ROWS, D),
            bf(ROWS, 256),
            bf(D, 768),
            bf(2, 1024, 256),
            bf(2, 1024, 256),
            f32(ROWS, 768),
            f32(2, ROWS, HEAD),
            f32(ROWS, HEAD),
            f32(ROWS, HEAD),
            bf(ROWS, 512),
            bf(*half),
            bf(*tall),
            bf(*half),
            bf(*half),
            bf(*tall),
            bf(*half),
            bf(*half),
            bf(*tall),
            bf(*half),
            bf(6, 128, 256),
            bf(6, 256, 128),
            bf(6, 128, 256),
            bf(8, 16, 256),
            bf(8, 32, 128),
            bf(8, 16, 256),
            bf(7, 16, 256),
            bf(7, 32, 128),
            bf(7, 16, 256),
            bf(8, 16, 256),
            bf(2, 16, 128),
            bf(8, 16, 128),
            bf(8, 16, 256),
            bf(128, 256),
            bf(256, 128),
            bf(128, 256),
            bf(8, 16, 256),
            bf(8, 16, 256),
            bf(16, 16, 128),
            f32(16, 8, 128),
            pltpu.SemaphoreType.DMA((SEMS,)),
            pltpu.SemaphoreType.DMA((5,)),
        ],
        compiler_params=pltpu.CompilerParams(collective_id=0, has_side_effects=True),
        name="attention_backward",
    )(
        seq_start,
        doc_lengths,
        jnp.asarray(inverse),
        row_lse.T,
        hidden_in,
        out_grad,
        attn_saved,
        w_qkv,
        w_out_t,
    )
    input_grad, grad_update, norm = pl.pallas_call(
        finish,
        out_shape=(
            jax.ShapeDtypeStruct((ROWS, D), BF16),
            jax.ShapeDtypeStruct((128, 768), F32),
            jax.ShapeDtypeStruct((1, 1), F32),
        ),
        in_specs=[vmem] * 3,
        out_specs=(hbm, vmem, vmem),
        scratch_shapes=[pltpu.SemaphoreType.DMA],
        compiler_params=pltpu.CompilerParams(vmem_limit_bytes=8 * 2**20),
        name="scaled_outputs",
    )(input_grad, grads, tiles)
    return (input_grad, grad_update, norm[0, 0])


def solution(mesh):
    split = Mesh(mesh.devices.reshape(8, 2, 4, 8, 2), AXES)
    tokens = P(FSDP_REP, None)
    in_specs = (tokens, tokens, tokens, tokens, P(FSDP, None), P(FSDP, None), tokens, P(FSDP_REP))
    out_specs = (tokens, P(FSDP, None), P())
    return jax.shard_map(body, mesh=split, in_specs=in_specs, out_specs=out_specs, check_vma=False)
```

```python
import jax
import jax.numpy as jnp
import numpy as np
from jax import lax
from jax.experimental import pallas as pl
from jax.experimental.pallas import tpu as pltpu
from jax.sharding import Mesh
from jax.sharding import PartitionSpec as P

D = 2048
HEAD = 128
ROWS = 256
AXES = ("fsdp_0", "fsdp_1", "rep_0", "rep_1", "rep_2")
FSDP = AXES[:2]
FSDP_REP = AXES
F32 = jnp.float32
BF16 = jnp.bfloat16
SEMS = 540


def mod(value, size):
    return lax.rem(value + size, size)


def dot(left, right, contract=((1,), (0,))):
    return lax.dot_general(left, right, (contract, ((), ())), preferred_element_type=F32)


class Links:
    def __init__(self, sems):
        self.sems, self.used, self.started = sems, 0, []

    def send(self, src, dst, device):
        at = self.used
        self.used += 2
        copy = pltpu.make_async_remote_copy(
            src_ref=src,
            dst_ref=dst,
            send_sem=self.sems.at[at],
            recv_sem=self.sems.at[at + 1],
            device_id=device,
            device_id_type=pl.DeviceIdType.MESH,
        )
        copy.start()
        self.started.append(copy)
        return copy

    def finish(self):
        for copy in self.started:
            copy.wait_send()


def arrived(copies):
    for copy in copies:
        copy.wait_recv()


def kernel(
    start_ref,
    doc_ref,
    inv_ref,
    lse_ref,
    hid_hbm,
    og_hbm,
    as_hbm,
    wq_hbm,
    wo_hbm,
    ig_ref,
    grads_ref,
    norm_ref,
    hid,
    og,
    saved,
    wbuf,
    hid_t,
    og_t,
    proj,
    lse,
    cos_ref,
    sin_ref,
    dqkv,
    gs_y,
    gs_x,
    gs_z,
    gr_y,
    gr_x,
    gr_z,
    s_y,
    s_x,
    s_z,
    r_y,
    r_x,
    r_z,
    s2_y,
    s2_x,
    s2_z,
    r2_y,
    r2_x,
    r2_z,
    r3_y,
    s3_x,
    r3_x,
    r3_z,
    far_y,
    far_x,
    far_z,
    fy,
    fz,
    fx,
    nz,
    nx,
    ny,
    sems,
    local,
    chain,
):
    y = lax.axis_index(AXES[0])
    zh = lax.axis_index(AXES[1])
    zl = lax.axis_index(AXES[2])
    x = lax.axis_index(AXES[3])
    c = lax.axis_index(AXES[4])
    z = zh * 4 + zl
    mate = (y, zh, zl, x, 1 - c)
    mirror = (y, 1 - zh, 3 - zl, x, c)

    def at_y(d):
        return (mod(y + d, 8), zh, zl, x, c)

    def at_x(d, dc=0):
        return (y, zh, zl, mod(x + d, 8), mod(c + dc, 2))

    def at_z(d, dc=0):
        there = mod(z + d, 8)
        return (y, there // 4, lax.rem(there, 4), x, mod(c + dc, 2))

    def at_zl(d, dc):
        return (y, zh, mod(zl + d, 4), x, mod(c + dc, 2))

    def rows_of(block, first, count):
        return pl.ds(pl.multiple_of(block * 128 + first, 16), count)

    own = y * 2 + zh
    own_rows = rows_of(own, 0, 128)
    load_wq = pltpu.make_async_copy(wq_hbm, wbuf.at[own_rows, pl.ds(0, 512)], local.at[0])
    load_wo = pltpu.make_async_copy(wo_hbm, wbuf.at[own_rows, pl.ds(512, 256)], local.at[1])
    load_og = pltpu.make_async_copy(og_hbm, og, local.at[2])
    load_as = pltpu.make_async_copy(as_hbm, saved, local.at[3])
    load_hid = pltpu.make_async_copy(hid_hbm, hid, local.at[4])
    for copy in (load_wq, load_wo, load_og, load_as, load_hid):
        copy.start()
    near = [mate, mirror]
    for at in (at_y, at_x, at_z):
        near += [at(1), at(-1)]
    barrier = pltpu.get_barrier_semaphore()

    def tell(sem, device):
        pl.semaphore_signal(sem, inc=1, device_id=device, device_id_type=pl.DeviceIdType.MESH)

    for peer in near:
        tell(barrier, peer)

    load_wq.wait()
    load_wo.wait()
    pl.semaphore_wait(barrier, len(near))

    def hear(step):
        for i in range(4):
            pl.semaphore_wait(chain.at[step, i], 1)

    def pass_word(step):
        for i, device in enumerate((at_x(1), at_x(-1), at_z(1), at_z(-1))):
            tell(chain.at[step, i], device)

    pass_word(0)

    links = Links(sems)

    def weight(block, first, count, device):
        ref = wbuf.at[rows_of(block, first, count), :]
        return links.send(ref, ref, device)

    color = lax.rem(x, 2)
    base, other_base = color * 64 + c * 32, (1 - color) * 64 + c * 32
    along_y = (at_y(1), at_y(-1))
    along_x = (at_x(1), at_x(-1))
    shared = []

    class Ring:
        def __init__(self, zside):
            self.zside, self.beside = zside, {0: []}
            self.sent = {(w, u): self.piece(0, u, along_y[w]) for u in range(2) for w in range(2)}

        def block(self, d):
            return mod(y + d, 8) * 2 + self.zside

        def piece(self, d, u, device):
            return weight(self.block(d), base + 16 * u, 16, device)

        def hand_over(self, d, u, s):
            self.beside[s].append(self.piece(d, u, along_x[u]))

        def to_mate(self, d, first):
            shared.append(weight(self.block(d), first, 32, mate))

        def step(self, s):
            before, self.sent, self.beside[s] = self.sent, {}, []
            for (w, u), copy in before.items():
                copy.wait_recv()
                d = s if w else -s
                if s < 3 or (s == 3 and u == w):
                    self.sent[w, u] = self.piece(d, u, along_y[w])
                self.hand_over(d, u, s)
            self.mate_rows(s, base)

        def mate_rows(self, s, first):
            for d in {0: (0,), 4: (4,)}.get(s, (-s, s)):
                self.to_mate(d, first)

        def collect(self, s):
            arrived(self.beside[s])
            self.mate_rows(s, other_base)

    ring_a = Ring(zh)
    to_mirror = [weight(own, base + 16 * u, 16, mirror) for u in range(2)]

    positions = (start_ref[0] + lax.broadcasted_iota(jnp.int32, (ROWS, HEAD), 0)).astype(F32)
    angles = positions * inv_ref[...]
    sign = jnp.where(lax.broadcasted_iota(jnp.int32, (ROWS, HEAD), 1) < HEAD // 2, -1.0, 1.0)
    for h in range(2):
        lse[h] = jnp.broadcast_to(lse_ref[h : h + 1, :], (HEAD, ROWS)).T
    cos_ref[...] = jnp.cos(angles)
    sin_ref[...] = jnp.sin(angles) * sign

    def transpose(src, dst, j):
        part = src[:, 256 * j : 256 * (j + 1)].T
        for i in range(2):
            for h in range(2):
                b = 2 * j + i
                dst[h, b * 64 : (b + 1) * 64, :] = part[i * 128 + h * 64 : i * 128 + h * 64 + 64]

    ring_a.step(1)
    hear(0)
    pass_word(1)
    load_og.wait()
    load_as.wait()
    for j in range(8):
        transpose(og, og_t, j)
    arrived(to_mirror)
    ring_b = Ring(1 - zh)
    for u in range(2):
        ring_b.hand_over(0, u, 0)
    ring_b.mate_rows(0, base)
    ring_a.step(2)
    hear(1)
    pass_word(2)

    sign_c = 1 - 2 * c

    class First:
        def __init__(self, chunks, parts, relay, me, at):
            self.chunks, self.parts, self.relay, self.me, self.at = chunks, parts, relay, me, at
            self.far = links.send(chunks.at[mod(me + 4, 8)], relay, at(sign_c))
            self.sent = [self.go(i, d) for i, d in enumerate((-3, 2, -2, 1, -1))]

        def go(self, i, d):
            there = mod(self.me + sign_c * d, 8)
            return links.send(self.chunks.at[there], self.parts.at[i], self.at(sign_c * d))

        def pass_on(self):
            self.far.wait_recv()
            there = mod(self.me + sign_c * 3, 8)
            both = self.chunks[there].astype(F32) + self.relay[...].astype(F32)
            self.chunks[there] = both.astype(BF16)
            self.sent.append(self.go(5, 3))

        def total(self):
            arrived(self.sent)
            return summed(self.chunks[self.me], self.parts, 6).astype(BF16)

    def summed(own_part, parts, count):
        total = own_part.astype(F32)
        for i in range(count):
            total = total + parts[i].astype(F32)
        return total

    def in_order(parts):
        total = parts[0].astype(F32)
        for i in range(1, 8):
            total = total + parts[i].astype(F32)
        return total

    def put_z(dst, block, tile):
        for qr in range(4):
            zz = (block % 2) * 4 + qr
            yy = block // 2
            dst[zz, yy * 16 : yy * 16 + 16, :] = tile[qr * 16 : qr * 16 + 16]

    def out_term(h, ch):
        return dot(og_t[h, ch * 256 : (ch + 1) * 256, :], saved[...])

    for ch in range(4):
        part = out_term(1 - c, ch).astype(BF16)
        for i in range(4):
            put_z(gs_z, ch * 4 + i, part[i * 64 : i * 64 + 64])
    core_z = links.send(gs_z, gr_z, mate)
    ring_a.collect(1)
    ring_a.step(3)
    ring_b.step(1)
    hear(2)
    for ch in range(4):
        part = out_term(c, ch)
        for i in range(4):
            put_z(s_z, ch * 4 + i, part[i * 64 : i * 64 + 64].astype(BF16))
    core_z.wait_recv()
    for k in range(8):
        s_z[k] = (s_z[k].astype(F32) + gr_z[k].astype(F32)).astype(BF16)
    first_z = First(s_z, r_z, far_z, z, at_z)
    ring_a.collect(2)
    ring_b.collect(0)
    ring_a.step(4)
    ring_b.step(2)
    load_hid.wait()
    for j in range(4):
        transpose(hid, hid_t, j)
    ring_a.collect(3)
    ring_b.collect(1)
    ring_b.step(3)
    first_z.pass_on()
    for j in range(4, 8):
        transpose(hid, hid_t, j)
    ring_a.collect(4)
    ring_b.collect(2)
    ring_b.step(4)
    ring_b.collect(3)
    ring_b.collect(4)
    arrived(shared)

    proj[:, :512] = dot(hid[...], wbuf[:, :512])
    proj[:, 512:] = dot(og[...], wbuf[:, 512:])
    cosine, sines = cos_ref[...], sin_ref[...]

    def rotary(value):
        return value * cosine + pltpu.roll(value, HEAD // 2, 1) * sines

    def rotary_back(value):
        return value * cosine - pltpu.roll(value, HEAD // 2, 1) * sines

    keys = rotary(proj[:, 256:384]).astype(BF16)
    values = proj[:, 384:512].astype(BF16)
    row = lax.broadcasted_iota(jnp.int32, (ROWS, ROWS), 0)
    col = lax.broadcasted_iota(jnp.int32, (ROWS, ROWS), 1)
    allowed = col <= row
    end = jnp.int32(0)
    for i in range(4):
        end = end + doc_ref[0, i]
        allowed = allowed & ((row >= end) == (col >= end))
    scale = 1.0 / HEAD**0.5
    key_grad = jnp.zeros((ROWS, HEAD), F32)
    value_grad = jnp.zeros((ROWS, HEAD), F32)
    for h in range(2):
        lanes = slice(h * HEAD, (h + 1) * HEAD)
        query = rotary(proj[:, lanes]).astype(BF16)
        grad = proj[:, 512 + h * HEAD : 512 + (h + 1) * HEAD].astype(BF16)
        scores = dot(query, keys, ((1,), (1,))) * scale
        probs = jnp.where(allowed, jnp.exp(scores - lse[h, :, 0:1]), 0.0)
        dprobs = dot(grad, values, ((1,), (1,)))
        delta = jnp.sum(
            grad.astype(F32) * saved[:, lanes].astype(F32), axis=1, keepdims=True
        )
        dscores = (probs * (dprobs - delta) * scale).astype(BF16)
        value_grad += dot(probs.astype(BF16), grad, ((0,), (0,)))
        key_grad += dot(dscores, query, ((0,), (0,)))
        dqkv[:, lanes] = rotary_back(dot(dscores, keys)).astype(BF16)
    dqkv[:, 256:384] = rotary_back(key_grad).astype(BF16)
    dqkv[:, 384:512] = value_grad.astype(BF16)

    def y_term(h, dst):
        for ch in range(4):
            part = dot(hid_t[h, ch * 256 : (ch + 1) * 256, :], dqkv[:, :256]).astype(BF16)
            for i in range(4):
                at, side = (ch * 4 + i) // 2, (i % 2) * 64
                dst[at, side : side + 64, :] = part[i * 64 : i * 64 + 64]

    def x_term(h, dst):
        for ch in range(4):
            part = dot(hid_t[h, ch * 256 : (ch + 1) * 256, :], dqkv[:, 256:]).astype(BF16)
            for i in range(4):
                at = (ch * 4 + i) * 16
                for qr in range(4):
                    for ct in range(2):
                        dst[qr * 2 + ct, at : at + 16, :] = part[
                            i * 64 + qr * 16 : i * 64 + qr * 16 + 16, ct * 128 : ct * 128 + 128
                        ]

    def add(dst, more):
        for k in range(8):
            dst[k] = (dst[k].astype(F32) + more[k].astype(F32)).astype(BF16)

    y_term(1 - c, gs_y)
    core_y = links.send(gs_y, gr_y, mate)
    x_term(1 - c, gs_x)
    core_x = links.send(gs_x, gr_x, mate)
    y_term(c, s_y)
    total = first_z.total()
    for k in range(8):
        s2_z[k] = total[k * 16 : k * 16 + 16]
    second_z = [links.send(s2_z.at[mod(y + d, 8)], r2_z.at[d - 1], at_y(d)) for d in range(1, 8)]
    core_y.wait_recv()
    add(s_y, gr_y)
    first_y = First(s_y, r_y, far_y, y, at_y)
    x_term(c, s_x)
    core_x.wait_recv()
    add(s_x, gr_x)
    first_x = First(s_x, r_x, far_x, x, at_x)

    for n in range(4):
        cols = slice(n * 512, (n + 1) * 512)
        ig_ref[:, cols] = dot(dqkv[...], wbuf[cols, :512], ((1,), (1,))).astype(BF16)
    first_y.pass_on()
    first_x.pass_on()

    arrived(second_z)
    r3_z[x] = summed(s2_z[y], r2_z, 7).astype(BF16)
    third_z = [links.send(r3_z.at[x], r3_z.at[x], at_x(d)) for d in range(1, 8)]

    total = first_y.total()
    for k in range(8):
        s2_y[k] = total[k * 16 : k * 16 + 16]
    second_y = [links.send(s2_y.at[mod(z + d, 8)], r2_y.at[d - 1], at_z(d)) for d in range(1, 8)]
    total = first_x.total()
    for k in range(8):
        s2_x[k] = total[k * 32 : k * 32 + 32]
    second_x = [links.send(s2_x.at[mod(y + d, 8)], r2_x.at[d - 1], at_y(d)) for d in range(1, 8)]

    def spread_zl(pieces):
        return [
            links.send(pieces.at[mine], pieces.at[mine], at_zl(d, dc) if d else mate)
            for d in range(4)
            for dc in range(2)
            if d or dc
        ]

    mine = c * 4 + zl
    arrived(third_z)
    fz[mine] = in_order(r3_z).astype(BF16)
    spread = spread_zl(fz)

    arrived(second_y)
    r3_y[x] = summed(s2_y[z], r2_y, 7).astype(BF16)
    third_y = [links.send(r3_y.at[x], r3_y.at[x], at_x(d)) for d in range(1, 8)]
    arrived(second_x)
    r3_x[z] = summed(s2_x[y], r2_x, 7).astype(BF16)
    third_x = [links.send(r3_x.at[z], r3_x.at[z], at_z(d)) for d in range(1, 8)]

    def squares(*pieces):
        rows = [jnp.sum(piece * piece, axis=0, keepdims=True) for piece in pieces]
        lanes = [row[:, i : i + 128] for row in rows for i in range(0, row.shape[1], 128)]
        return sum(lanes[1:], lanes[0])

    arrived(third_y)
    fy[mine] = in_order(r3_y).astype(BF16)
    slot = c * 8 + z
    nz[slot] = squares(fy[mine].astype(F32), fz[mine].astype(F32))
    spread += [
        links.send(nz.at[slot], nz.at[slot], at_z(d, dc) if d else mate)
        for d in range(8)
        for dc in range(2)
        if d or dc
    ]
    spread += spread_zl(fy)
    arrived(third_x)
    tile = c * 8 + x
    both = in_order(r3_x).astype(BF16)
    s3_x[0], s3_x[1] = both[:16], both[16:]
    fx[tile] = s3_x[zh]
    nx[tile] = squares(both.astype(F32))
    for part in (nx, fx):
        spread += [
            links.send(part.at[tile], part.at[tile], at_x(d, dc) if d else mate)
            for d in range(8)
            for dc in range(2)
            if d or dc
        ]
    arrived(spread)
    total = nz[0] + nx[0]
    for i in range(1, 16):
        total = total + (nz[i] + nx[i])
    ny[y] = total
    along = [links.send(ny.at[y], ny.at[y], at_y(d)) for d in range(1, 8)]
    for i in range(8):
        grads_ref[i * 16 : i * 16 + 16, 0:256] = fy[i].astype(F32)
        grads_ref[i * 16 : i * 16 + 16, 512:768] = fz[i].astype(F32)
        for ct in range(2):
            at = (i // 4) * 8 + (i % 4) * 2 + ct
            grads_ref[i * 16 : i * 16 + 16, 256 + ct * 128 : 384 + ct * 128] = fx[at].astype(F32)
    arrived(along)
    total = ny[0]
    for i in range(1, 8):
        total = total + ny[i]
    norm_ref[...] = total
    links.finish()
    assert links.used <= SEMS, links.used


def finish(ig_ref, grads_ref, tiles_ref, ig_out, update_ref, norm_ref, sem):
    store = pltpu.make_async_copy(ig_ref, ig_out, sem)
    store.start()
    norm_sq = jnp.sum(tiles_ref[...], axis=1, keepdims=True)
    update_ref[...] = grads_ref[...] * lax.rsqrt(norm_sq / (D * 768) + 1e-06)
    norm_ref[...] = jnp.sqrt(norm_sq)
    store.wait()


def body(hidden_in, out_grad, attn_saved, row_lse, w_qkv, w_out_t, doc_lengths, seq_start):
    power = np.arange(HEAD // 2, dtype=np.float64) * 2.0 / HEAD
    inverse = np.tile(1000000.0 ** (-power), 2).astype(np.float32)[None, :]
    smem = pl.BlockSpec(memory_space=pltpu.SMEM)
    vmem = pl.BlockSpec(memory_space=pltpu.VMEM)
    hbm = pl.BlockSpec(memory_space=pl.ANY)
    half = (8, 128, 256)
    tall = (8, 256, 128)

    def bf(*shape):
        return pltpu.VMEM(shape, BF16)

    def f32(*shape):
        return pltpu.VMEM(shape, F32)

    input_grad, grads, tiles = pl.pallas_call(
        kernel,
        out_shape=(bf(ROWS, D), f32(128, 768), f32(1, 128)),
        in_specs=[smem, smem, vmem, vmem, hbm, hbm, hbm, hbm, hbm],
        out_specs=(vmem, vmem, vmem),
        scratch_shapes=[
            bf(ROWS, D),
            bf(ROWS, D),
            bf(ROWS, 256),
            bf(D, 768),
            bf(2, 1024, 256),
            bf(2, 1024, 256),
            f32(ROWS, 768),
            f32(2, ROWS, HEAD),
            f32(ROWS, HEAD),
            f32(ROWS, HEAD),
            bf(ROWS, 512),
            bf(*half),
            bf(*tall),
            bf(*half),
            bf(*half),
            bf(*tall),
            bf(*half),
            bf(*half),
            bf(*tall),
            bf(*half),
            bf(6, 128, 256),
            bf(6, 256, 128),
            bf(6, 128, 256),
            bf(8, 16, 256),
            bf(8, 32, 128),
            bf(8, 16, 256),
            bf(7, 16, 256),
            bf(7, 32, 128),
            bf(7, 16, 256),
            bf(8, 16, 256),
            bf(2, 16, 128),
            bf(8, 32, 128),
            bf(8, 16, 256),
            bf(128, 256),
            bf(256, 128),
            bf(128, 256),
            bf(8, 16, 256),
            bf(8, 16, 256),
            bf(16, 16, 128),
            f32(16, 1, 128),
            f32(16, 1, 128),
            f32(8, 1, 128),
            pltpu.SemaphoreType.DMA((SEMS,)),
            pltpu.SemaphoreType.DMA((5,)),
            pltpu.SemaphoreType.REGULAR((3, 4)),
        ],
        compiler_params=pltpu.CompilerParams(collective_id=0, has_side_effects=True),
        name="attention_backward",
    )(
        seq_start,
        doc_lengths,
        jnp.asarray(inverse),
        row_lse.T,
        hidden_in,
        out_grad,
        attn_saved,
        w_qkv,
        w_out_t,
    )
    input_grad, grad_update, norm = pl.pallas_call(
        finish,
        out_shape=(
            jax.ShapeDtypeStruct((ROWS, D), BF16),
            jax.ShapeDtypeStruct((128, 768), F32),
            jax.ShapeDtypeStruct((1, 1), F32),
        ),
        in_specs=[vmem] * 3,
        out_specs=(hbm, vmem, vmem),
        scratch_shapes=[pltpu.SemaphoreType.DMA],
        compiler_params=pltpu.CompilerParams(vmem_limit_bytes=8 * 2**20),
        name="scaled_outputs",
    )(input_grad, grads, tiles)
    return (input_grad, grad_update, norm[0, 0])


def solution(mesh):
    split = Mesh(mesh.devices.reshape(8, 2, 4, 8, 2), AXES)
    tokens = P(FSDP_REP, None)
    in_specs = (tokens, tokens, tokens, tokens, P(FSDP, None), P(FSDP, None), tokens, P(FSDP_REP))
    out_specs = (tokens, P(FSDP, None), P())
    return jax.shard_map(body, mesh=split, in_specs=in_specs, out_specs=out_specs, check_vma=False)
```

```python
import jax
import jax.numpy as jnp
import numpy as np
from jax import lax
from jax.experimental import pallas as pl
from jax.experimental.pallas import tpu as pltpu
from jax.sharding import Mesh
from jax.sharding import PartitionSpec as P

D = 2048
HEAD = 128
ROWS = 256
AXES = ("fsdp_0", "fsdp_1", "rep_0", "rep_1", "rep_2")
FSDP = AXES[:2]
FSDP_REP = AXES
F32 = jnp.float32
BF16 = jnp.bfloat16
SEMS = 81


def mod(value, size):
    return lax.rem(value + size, size)


def dot(left, right, contract=((1,), (0,))):
    return lax.dot_general(left, right, (contract, ((), ())), preferred_element_type=F32)


MESH = pl.DeviceIdType.MESH


class Flags:
    def __init__(self, sems):
        self.sems, self.used = sems, 0

    def take(self):
        self.used += 1
        return self.sems.at[self.used - 1]


def start(src, dst, device, sent, got):
    pltpu.make_async_remote_copy(
        src_ref=src, dst_ref=dst, send_sem=sent, recv_sem=got, device_id=device, device_id_type=MESH
    ).start()


def await_bytes(whole, count, flag):
    ref = whole.at[pl.ds(0, count)]
    pltpu.make_async_copy(ref, ref, flag).wait()


class Batch:
    def __init__(self, flags, whole):
        self.whole, self.sent, self.got, self.count = whole, flags.take(), flags.take(), 0

    def send(self, src, dst, device, units=1):
        start(src, dst, device, self.sent, self.got)
        self.count += units
        return self

    def arrived(self):
        await_bytes(self.whole, self.count, self.got)

    def left(self):
        await_bytes(self.whole, self.count, self.sent)


def kernel(
    start_hbm,
    doc_hbm,
    inv_hbm,
    lse_hbm,
    hid_hbm,
    og_hbm,
    as_hbm,
    wq_hbm,
    wo_hbm,
    ig_ref,
    grads_ref,
    norm_ref,
    start_ref,
    doc_ref,
    inv_ref,
    lse_ref,
    hid,
    og,
    saved,
    wbuf,
    hid_t,
    og_t,
    proj,
    lse,
    cos_ref,
    sin_ref,
    dqkv,
    gs_y,
    gs_x,
    gs_z,
    gr_y,
    gr_x,
    gr_z,
    s_y,
    s_x,
    s_z,
    r_y,
    r_x,
    r_z,
    s2_y,
    s2_x,
    s2_z,
    r2_y,
    r2_x,
    r2_z,
    r3_y,
    s3_x,
    r3_x,
    r3_z,
    far_y,
    far_x,
    far_z,
    fy,
    fz,
    fx,
    nz,
    nx,
    ny,
    sems,
    local,
    chain,
):
    y = lax.axis_index(AXES[0])
    zh = lax.axis_index(AXES[1])
    zl = lax.axis_index(AXES[2])
    x = lax.axis_index(AXES[3])
    c = lax.axis_index(AXES[4])
    z = zh * 4 + zl
    mate = (y, zh, zl, x, 1 - c)
    mirror = (y, 1 - zh, 3 - zl, x, c)

    def at_y(d):
        return (mod(y + d, 8), zh, zl, x, c)

    def at_x(d, dc=0):
        return (y, zh, zl, mod(x + d, 8), mod(c + dc, 2))

    def at_z(d, dc=0):
        there = mod(z + d, 8)
        return (y, there // 4, lax.rem(there, 4), x, mod(c + dc, 2))

    def at_zl(d, dc):
        return (y, zh, mod(zl + d, 4), x, mod(c + dc, 2))

    def rows_of(block, first, count):
        return pl.ds(pl.multiple_of(block * 128 + first, 16), count)

    own = y * 2 + zh
    own_rows = rows_of(own, 0, 128)
    load_wq = pltpu.make_async_copy(wq_hbm, wbuf.at[own_rows, pl.ds(0, 512)], local.at[0])
    load_wo = pltpu.make_async_copy(wo_hbm, wbuf.at[own_rows, pl.ds(512, 256)], local.at[1])
    load_og = pltpu.make_async_copy(og_hbm, og, local.at[2])
    load_as = pltpu.make_async_copy(as_hbm, saved, local.at[3])
    load_hid = pltpu.make_async_copy(hid_hbm, hid, local.at[4])
    small = [
        pltpu.make_async_copy(src, dst, local.at[5 + i])
        for i, (src, dst) in enumerate(
            ((start_hbm, start_ref), (inv_hbm, inv_ref), (lse_hbm, lse_ref), (doc_hbm, doc_ref))
        )
    ]
    for copy in (load_wq, load_wo, *small, load_og, load_as, load_hid):
        copy.start()
    near = [mate, mirror]
    for at in (at_y, at_x, at_z):
        near += [at(1), at(-1)]
    barrier = pltpu.get_barrier_semaphore()

    def tell(sem, device):
        pl.semaphore_signal(sem, inc=1, device_id=device, device_id_type=MESH)

    for peer in near:
        tell(barrier, peer)

    load_wq.wait()
    load_wo.wait()
    pl.semaphore_wait(barrier, len(near))

    def hear(step):
        for i in range(4):
            pl.semaphore_wait(chain.at[step, i], 1)

    def pass_word(step):
        for i, device in enumerate((at_x(1), at_x(-1), at_z(1), at_z(-1))):
            tell(chain.at[step, i], device)

    pass_word(0)

    flags = Flags(sems)
    weights_sent = flags.take()
    rows_sent = []

    def weight(block, first, count, device, got):
        ref = wbuf.at[rows_of(block, first, count), :]
        start(ref, ref, device, weights_sent, got)
        rows_sent.append(count)

    color = lax.rem(x, 2)
    base, other_base = color * 64 + c * 32, (1 - color) * 64 + c * 32
    along_y = {s: (at_y(s), at_y(-s)) for s in (1, 2)}
    along_x = (at_x(1), at_x(-1))
    across_x = (at_x(1, 1), at_x(-1, 1))
    near_rows, far_rows = [], []
    shared = [(flags.take(), near_rows)] * 3 + [(flags.take(), far_rows)] * 2

    class Ring:
        def __init__(self, zside, leap):
            self.zside, self.leap = zside, leap
            self.due = {s: {} for s in range(1, 5)}
            self.beside = {s: (flags.take(), []) for s in range(5)}
            for u in range(2):
                for w in range(2):
                    for s in (2, 1) if leap else (1,):
                        self.piece(0, u, w, s, s)

        def block(self, d):
            return mod(y + d, 8) * 2 + self.zside

        def piece(self, d, u, w, s, hop):
            self.due[s][w, u] = flags.take()
            weight(self.block(d), base + 16 * u, 16, along_y[hop][w], self.due[s][w, u])

        def hand_over(self, d, u, s):
            got, rows = self.beside[s]
            for device in (along_x[u], across_x[u]) if s == 4 else (along_x[u],):
                weight(self.block(d), base + 16 * u, 16, device, got)
                rows.append(16)

        def to_mate(self, d, first):
            got, rows = shared[abs(d)]
            weight(self.block(d), first, 32, mate, got)
            rows.append(32)

        def step(self, s):
            for (w, u), got in self.due[s].items():
                await_bytes(wbuf, 16, got)
                d = s if w else -s
                if self.leap and s == 2:
                    if u == w:
                        self.piece(d, u, w, 4, 2)
                    self.piece(d, u, w, 3, 1)
                elif not self.leap and (s < 3 or (s == 3 and u == w)):
                    self.piece(d, u, w, s + 1, 1)
                self.hand_over(d, u, s)
            self.mate_rows(s, base)

        def mate_rows(self, s, first):
            for d in {0: (0,), 4: (4,)}.get(s, (-s, s)):
                self.to_mate(d, first)

        def collect(self, s):
            got, rows = self.beside[s]
            await_bytes(wbuf, sum(rows), got)
            if s < 4:
                self.mate_rows(s, other_base)

    ring_a = Ring(zh, False)
    from_mirror = flags.take()
    weight(own, base, 32, mirror, from_mirror)

    for copy in small:
        copy.wait()
    positions = (start_ref[0] + lax.broadcasted_iota(jnp.int32, (ROWS, HEAD), 0)).astype(F32)
    angles = positions * inv_ref[...]
    sign = jnp.where(lax.broadcasted_iota(jnp.int32, (ROWS, HEAD), 1) < HEAD // 2, -1.0, 1.0)
    for h in range(2):
        lse[h] = jnp.broadcast_to(lse_ref[h : h + 1, :], (HEAD, ROWS)).T
    cos_ref[...] = jnp.cos(angles)
    sin_ref[...] = jnp.sin(angles) * sign

    def transpose(src, dst, j):
        part = src[:, 256 * j : 256 * (j + 1)].T
        for i in range(2):
            for h in range(2):
                b = 2 * j + i
                dst[h, b * 64 : (b + 1) * 64, :] = part[i * 128 + h * 64 : i * 128 + h * 64 + 64]

    ring_a.step(1)
    hear(0)
    pass_word(1)
    load_og.wait()
    load_as.wait()
    for j in range(8):
        transpose(og, og_t, j)
    await_bytes(wbuf, 32, from_mirror)
    ring_b = Ring(1 - zh, True)
    for u in range(2):
        ring_b.hand_over(0, u, 0)
    ring_b.mate_rows(0, base)
    ring_a.step(2)
    hear(1)
    pass_word(2)

    sign_c = 1 - 2 * c

    class First:
        def __init__(self, chunks, parts, relay, me, at):
            self.chunks, self.parts, self.relay, self.me, self.at = chunks, parts, relay, me, at
            self.sent, self.got, self.far = flags.take(), flags.take(), flags.take()
            start(chunks.at[mod(me + 4, 8)], relay, at(sign_c), self.sent, self.far)
            for i, d in enumerate((-3, 2, -2, 1, -1)):
                self.go(i, d)

        def go(self, i, d):
            there = mod(self.me + sign_c * d, 8)
            start(self.chunks.at[there], self.parts.at[i], self.at(sign_c * d), self.sent, self.got)

        def pass_on(self):
            await_bytes(self.chunks, 1, self.far)
            there = mod(self.me + sign_c * 3, 8)
            both = self.chunks[there].astype(F32) + self.relay[...].astype(F32)
            self.chunks[there] = both.astype(BF16)
            self.go(5, 3)

        def total(self):
            await_bytes(self.chunks, 6, self.got)
            return summed(self.chunks[self.me], self.parts, 6).astype(BF16)

        def left(self):
            await_bytes(self.chunks, 7, self.sent)

    def summed(own_part, parts, count):
        total = own_part.astype(F32)
        for i in range(count):
            total = total + parts[i].astype(F32)
        return total

    def in_order(parts):
        total = parts[0].astype(F32)
        for i in range(1, 8):
            total = total + parts[i].astype(F32)
        return total

    def put_z(dst, block, tile):
        for qr in range(4):
            zz = (block % 2) * 4 + qr
            yy = block // 2
            dst[zz, yy * 16 : yy * 16 + 16, :] = tile[qr * 16 : qr * 16 + 16]

    def out_term(h, ch):
        return dot(og_t[h, ch * 256 : (ch + 1) * 256, :], saved[...])

    for ch in range(4):
        part = out_term(1 - c, ch).astype(BF16)
        for i in range(4):
            put_z(gs_z, ch * 4 + i, part[i * 64 : i * 64 + 64])
    core_z = Batch(flags, gs_z).send(gs_z, gr_z, mate, 8)
    ring_a.collect(1)
    ring_b.step(1)
    ring_b.step(2)
    ring_a.step(3)
    hear(2)
    for ch in range(4):
        part = out_term(c, ch)
        for i in range(4):
            put_z(s_z, ch * 4 + i, part[i * 64 : i * 64 + 64].astype(BF16))
    core_z.arrived()
    for k in range(8):
        s_z[k] = (s_z[k].astype(F32) + gr_z[k].astype(F32)).astype(BF16)
    first_z = First(s_z, r_z, far_z, z, at_z)
    ring_a.collect(2)
    ring_b.collect(0)
    ring_b.collect(1)
    ring_b.step(3)
    ring_a.step(4)
    load_hid.wait()
    for j in range(4):
        transpose(hid, hid_t, j)
    ring_b.step(4)
    ring_b.collect(2)
    ring_a.collect(3)
    first_z.pass_on()
    for j in range(4, 8):
        transpose(hid, hid_t, j)
    ring_b.collect(3)
    await_bytes(wbuf, sum(near_rows), shared[0][0])

    def project(d, first=False):
        rows = pl.ds(pl.multiple_of(mod(y + d, 8) * 256, 256), 256)
        for src, cols in ((hid, slice(0, 512)), (og, slice(512, 768))):
            part = dot(src[:, rows], wbuf[rows, cols])
            proj[:, cols] = part if first else proj[:, cols] + part

    project(0, True)
    for d in (1, -1, 2, -2):
        project(d)
    ring_a.collect(4)
    ring_b.collect(4)
    await_bytes(wbuf, sum(far_rows), shared[4][0])
    for d in (3, -3, 4):
        project(d)
    cosine, sines = cos_ref[...], sin_ref[...]

    def rotary(value):
        return value * cosine + pltpu.roll(value, HEAD // 2, 1) * sines

    def rotary_back(value):
        return value * cosine - pltpu.roll(value, HEAD // 2, 1) * sines

    keys = rotary(proj[:, 256:384]).astype(BF16)
    values = proj[:, 384:512].astype(BF16)
    row = lax.broadcasted_iota(jnp.int32, (ROWS, ROWS), 0)
    col = lax.broadcasted_iota(jnp.int32, (ROWS, ROWS), 1)
    allowed = col <= row
    end = jnp.int32(0)
    for i in range(4):
        end = end + doc_ref[0, i]
        allowed = allowed & ((row >= end) == (col >= end))
    scale = 1.0 / HEAD**0.5
    key_grad = jnp.zeros((ROWS, HEAD), F32)
    value_grad = jnp.zeros((ROWS, HEAD), F32)
    for h in range(2):
        lanes = slice(h * HEAD, (h + 1) * HEAD)
        query = rotary(proj[:, lanes]).astype(BF16)
        grad = proj[:, 512 + h * HEAD : 512 + (h + 1) * HEAD].astype(BF16)
        scores = dot(query, keys, ((1,), (1,))) * scale
        probs = jnp.where(allowed, jnp.exp(scores - lse[h, :, 0:1]), 0.0)
        dprobs = dot(grad, values, ((1,), (1,)))
        delta = jnp.sum(
            grad.astype(F32) * saved[:, lanes].astype(F32), axis=1, keepdims=True
        )
        dscores = (probs * (dprobs - delta) * scale).astype(BF16)
        value_grad += dot(probs.astype(BF16), grad, ((0,), (0,)))
        key_grad += dot(dscores, query, ((0,), (0,)))
        dqkv[:, lanes] = rotary_back(dot(dscores, keys)).astype(BF16)
    dqkv[:, 256:384] = rotary_back(key_grad).astype(BF16)
    dqkv[:, 384:512] = value_grad.astype(BF16)

    def y_term(h, dst):
        for ch in range(4):
            part = dot(hid_t[h, ch * 256 : (ch + 1) * 256, :], dqkv[:, :256]).astype(BF16)
            for i in range(4):
                at, side = (ch * 4 + i) // 2, (i % 2) * 64
                dst[at, side : side + 64, :] = part[i * 64 : i * 64 + 64]

    def x_term(h, dst):
        for ch in range(4):
            part = dot(hid_t[h, ch * 256 : (ch + 1) * 256, :], dqkv[:, 256:]).astype(BF16)
            for i in range(4):
                at = (ch * 4 + i) * 16
                for qr in range(4):
                    for ct in range(2):
                        dst[qr * 2 + ct, at : at + 16, :] = part[
                            i * 64 + qr * 16 : i * 64 + qr * 16 + 16, ct * 128 : ct * 128 + 128
                        ]

    def add(dst, more):
        for k in range(8):
            dst[k] = (dst[k].astype(F32) + more[k].astype(F32)).astype(BF16)

    y_term(1 - c, gs_y)
    core_y = Batch(flags, gs_y).send(gs_y, gr_y, mate, 8)
    x_term(1 - c, gs_x)
    core_x = Batch(flags, gs_x).send(gs_x, gr_x, mate, 8)
    y_term(c, s_y)
    def exchange(parts, landing, me, at):
        batch = Batch(flags, parts)
        for d in range(1, 8):
            batch.send(parts.at[mod(me + d, 8)], landing.at[d - 1], at(d))
        return batch

    def broadcast(pieces, me, devices):
        batch = Batch(flags, pieces)
        for device in devices:
            batch.send(pieces.at[me], pieces.at[me], device)
        return batch

    total = first_z.total()
    for k in range(8):
        s2_z[k] = total[k * 16 : k * 16 + 16]
    second_z = exchange(s2_z, r2_z, y, at_y)
    core_y.arrived()
    add(s_y, gr_y)
    first_y = First(s_y, r_y, far_y, y, at_y)
    x_term(c, s_x)
    core_x.arrived()
    add(s_x, gr_x)
    first_x = First(s_x, r_x, far_x, x, at_x)

    for n in range(4):
        cols = slice(n * 512, (n + 1) * 512)
        ig_ref[:, cols] = dot(dqkv[...], wbuf[cols, :512], ((1,), (1,))).astype(BF16)
    first_y.pass_on()
    first_x.pass_on()

    await_bytes(wbuf, sum(rows_sent), weights_sent)
    for batch in (core_z, core_y, core_x, first_z, second_z):
        batch.left()
    second_z.arrived()
    r3_z[x] = summed(s2_z[y], r2_z, 7).astype(BF16)
    third_z = broadcast(r3_z, x, [at_x(d) for d in range(1, 8)])

    total = first_y.total()
    for k in range(8):
        s2_y[k] = total[k * 16 : k * 16 + 16]
    second_y = exchange(s2_y, r2_y, z, at_z)
    total = first_x.total()
    for k in range(8):
        s2_x[k] = total[k * 32 : k * 32 + 32]
    second_x = exchange(s2_x, r2_x, y, at_y)

    beside_zl = [at_zl(d, dc) if d else mate for d in range(4) for dc in range(2) if d or dc]
    beside_z = [at_z(d, dc) if d else mate for d in range(8) for dc in range(2) if d or dc]
    beside_x = [at_x(d, dc) if d else mate for d in range(8) for dc in range(2) if d or dc]

    mine = c * 4 + zl
    third_z.arrived()
    fz[mine] = in_order(r3_z).astype(BF16)
    spread = [broadcast(fz, mine, beside_zl)]

    second_y.arrived()
    r3_y[x] = summed(s2_y[z], r2_y, 7).astype(BF16)
    third_y = broadcast(r3_y, x, [at_x(d) for d in range(1, 8)])
    second_x.arrived()
    r3_x[z] = summed(s2_x[y], r2_x, 7).astype(BF16)
    third_x = broadcast(r3_x, z, [at_z(d) for d in range(1, 8)])

    def squares(*pieces):
        rows = [jnp.sum(piece * piece, axis=0, keepdims=True) for piece in pieces]
        lanes = [row[:, i : i + 128] for row in rows for i in range(0, row.shape[1], 128)]
        return sum(lanes[1:], lanes[0])

    first_y.left()
    first_x.left()
    third_y.arrived()
    fy[mine] = in_order(r3_y).astype(BF16)
    slot = c * 8 + z
    nz[slot] = squares(fy[mine].astype(F32), fz[mine].astype(F32))
    spread.append(broadcast(nz, slot, beside_z))
    spread.append(broadcast(fy, mine, beside_zl))
    third_x.arrived()
    tile = c * 8 + x
    both = in_order(r3_x).astype(BF16)
    s3_x[0], s3_x[1] = both[:16], both[16:]
    fx[tile] = s3_x[zh]
    nx[tile] = squares(both.astype(F32))
    spread.append(broadcast(nx, tile, beside_x))
    spread.append(broadcast(fx, tile, beside_x))
    for batch in spread:
        batch.arrived()
    total = nz[0] + nx[0]
    for i in range(1, 16):
        total = total + (nz[i] + nx[i])
    ny[y] = total
    along = broadcast(ny, y, [at_y(d) for d in range(1, 8)])
    for i in range(8):
        grads_ref[i * 16 : i * 16 + 16, 0:256] = fy[i].astype(F32)
        grads_ref[i * 16 : i * 16 + 16, 512:768] = fz[i].astype(F32)
        for ct in range(2):
            at = (i // 4) * 8 + (i % 4) * 2 + ct
            grads_ref[i * 16 : i * 16 + 16, 256 + ct * 128 : 384 + ct * 128] = fx[at].astype(F32)
    for batch in (second_y, second_x, third_z, third_y, third_x, *spread):
        batch.left()
    along.arrived()
    total = ny[0]
    for i in range(1, 8):
        total = total + ny[i]
    norm_ref[...] = total
    along.left()
    assert flags.used <= SEMS, flags.used


def finish(ig_ref, grads_ref, tiles_ref, ig_out, update_ref, norm_ref, sem):
    store = pltpu.make_async_copy(ig_ref, ig_out, sem)
    store.start()
    norm_sq = jnp.sum(tiles_ref[...], axis=1, keepdims=True)
    update_ref[...] = grads_ref[...] * lax.rsqrt(norm_sq / (D * 768) + 1e-06)
    norm_ref[...] = jnp.sqrt(norm_sq)
    store.wait()


def body(hidden_in, out_grad, attn_saved, row_lse, w_qkv, w_out_t, doc_lengths, seq_start):
    power = np.arange(HEAD // 2, dtype=np.float64) * 2.0 / HEAD
    inverse = np.tile(1000000.0 ** (-power), 2).astype(np.float32)[None, :]
    vmem = pl.BlockSpec(memory_space=pltpu.VMEM)
    hbm = pl.BlockSpec(memory_space=pl.ANY)
    half = (8, 128, 256)
    tall = (8, 256, 128)

    def bf(*shape):
        return pltpu.VMEM(shape, BF16)

    def f32(*shape):
        return pltpu.VMEM(shape, F32)

    input_grad, grads, tiles = pl.pallas_call(
        kernel,
        out_shape=(bf(ROWS, D), f32(128, 768), f32(1, 128)),
        in_specs=[hbm] * 9,
        out_specs=(vmem, vmem, vmem),
        scratch_shapes=[
            pltpu.SMEM((1,), jnp.int32),
            pltpu.SMEM((1, 4), jnp.int32),
            f32(1, HEAD),
            f32(2, ROWS),
            bf(ROWS, D),
            bf(ROWS, D),
            bf(ROWS, 256),
            bf(D, 768),
            bf(2, 1024, 256),
            bf(2, 1024, 256),
            f32(ROWS, 768),
            f32(2, ROWS, HEAD),
            f32(ROWS, HEAD),
            f32(ROWS, HEAD),
            bf(ROWS, 512),
            bf(*half),
            bf(*tall),
            bf(*half),
            bf(*half),
            bf(*tall),
            bf(*half),
            bf(*half),
            bf(*tall),
            bf(*half),
            bf(6, 128, 256),
            bf(6, 256, 128),
            bf(6, 128, 256),
            bf(8, 16, 256),
            bf(8, 32, 128),
            bf(8, 16, 256),
            bf(7, 16, 256),
            bf(7, 32, 128),
            bf(7, 16, 256),
            bf(8, 16, 256),
            bf(2, 16, 128),
            bf(8, 32, 128),
            bf(8, 16, 256),
            bf(128, 256),
            bf(256, 128),
            bf(128, 256),
            bf(8, 16, 256),
            bf(8, 16, 256),
            bf(16, 16, 128),
            f32(16, 1, 128),
            f32(16, 1, 128),
            f32(8, 1, 128),
            pltpu.SemaphoreType.DMA((SEMS,)),
            pltpu.SemaphoreType.DMA((9,)),
            pltpu.SemaphoreType.REGULAR((3, 4)),
        ],
        compiler_params=pltpu.CompilerParams(collective_id=0, has_side_effects=True),
        name="attention_backward",
    )(
        seq_start,
        doc_lengths,
        jnp.asarray(inverse),
        row_lse.T,
        hidden_in,
        out_grad,
        attn_saved,
        w_qkv,
        w_out_t,
    )
    input_grad, grad_update, norm = pl.pallas_call(
        finish,
        out_shape=(
            jax.ShapeDtypeStruct((ROWS, D), BF16),
            jax.ShapeDtypeStruct((128, 768), F32),
            jax.ShapeDtypeStruct((1, 1), F32),
        ),
        in_specs=[vmem] * 3,
        out_specs=(hbm, vmem, vmem),
        scratch_shapes=[pltpu.SemaphoreType.DMA],
        compiler_params=pltpu.CompilerParams(vmem_limit_bytes=8 * 2**20),
        name="scaled_outputs",
    )(input_grad, grads, tiles)
    return (input_grad, grad_update, norm[0, 0])


def solution(mesh):
    split = Mesh(mesh.devices.reshape(8, 2, 4, 8, 2), AXES)
    tokens = P(FSDP_REP, None)
    in_specs = (tokens, tokens, tokens, tokens, P(FSDP, None), P(FSDP, None), tokens, P(FSDP_REP))
    out_specs = (tokens, P(FSDP, None), P())
    return jax.shard_map(body, mesh=split, in_specs=in_specs, out_specs=out_specs, check_vma=False)
```

```python
import jax
import jax.numpy as jnp
import numpy as np
from jax import lax
from jax.experimental import pallas as pl
from jax.experimental.pallas import tpu as pltpu
from jax.sharding import Mesh
from jax.sharding import PartitionSpec as P

D = 2048
HEAD = 128
ROWS = 256
AXES = ("fsdp_0", "fsdp_1", "rep_0", "rep_1", "rep_2")
FSDP = AXES[:2]
FSDP_REP = AXES
F32 = jnp.float32
BF16 = jnp.bfloat16
SEMS = 82
FAR_FIRST = (4, 3, 5, 2, 6, 1, 7)


def mod(value, size):
    return lax.rem(value + size, size)


def dot(left, right, contract=((1,), (0,))):
    return lax.dot_general(left, right, (contract, ((), ())), preferred_element_type=F32)


MESH = pl.DeviceIdType.MESH


class Flags:
    def __init__(self, sems):
        self.sems, self.used = sems, 0

    def take(self):
        self.used += 1
        return self.sems.at[self.used - 1]


def start(src, dst, device, sent, got):
    pltpu.make_async_remote_copy(
        src_ref=src, dst_ref=dst, send_sem=sent, recv_sem=got, device_id=device, device_id_type=MESH
    ).start()


def await_bytes(whole, count, flag):
    ref = whole.at[pl.ds(0, count)]
    pltpu.make_async_copy(ref, ref, flag).wait()


class Batch:
    def __init__(self, flags, whole):
        self.whole, self.sent, self.got, self.count = whole, flags.take(), flags.take(), 0

    def send(self, src, dst, device, units=1):
        start(src, dst, device, self.sent, self.got)
        self.count += units
        return self

    def arrived(self):
        await_bytes(self.whole, self.count, self.got)

    def left(self):
        await_bytes(self.whole, self.count, self.sent)


def kernel(
    start_hbm,
    doc_hbm,
    inv_hbm,
    lse_hbm,
    hid_hbm,
    og_hbm,
    as_hbm,
    wq_hbm,
    wo_hbm,
    ig_ref,
    grads_ref,
    norm_ref,
    start_ref,
    doc_ref,
    inv_ref,
    lse_ref,
    hid,
    og,
    saved,
    wbuf,
    hid_t,
    og_t,
    proj,
    lse,
    cos_ref,
    sin_ref,
    dqkv,
    gs_y,
    gs_x,
    gs_z,
    gr_y,
    gr_x,
    gr_z,
    s_y,
    s_x,
    s_z,
    r_y,
    r_x,
    r_z,
    s2_y,
    s2_x,
    s2_z,
    r2_y,
    r2_x,
    r2_z,
    r3_y,
    s3_x,
    r3_x,
    r3_z,
    far_y,
    far_x,
    far_z,
    fy,
    fz,
    fx,
    nz,
    nx,
    ny,
    sems,
    local,
    chain,
):
    y = lax.axis_index(AXES[0])
    zh = lax.axis_index(AXES[1])
    zl = lax.axis_index(AXES[2])
    x = lax.axis_index(AXES[3])
    c = lax.axis_index(AXES[4])
    z = zh * 4 + zl
    mate = (y, zh, zl, x, 1 - c)
    mirror = (y, 1 - zh, 3 - zl, x, c)

    def at_y(d):
        return (mod(y + d, 8), zh, zl, x, c)

    def at_x(d, dc=0):
        return (y, zh, zl, mod(x + d, 8), mod(c + dc, 2))

    def at_z(d, dc=0):
        there = mod(z + d, 8)
        return (y, there // 4, lax.rem(there, 4), x, mod(c + dc, 2))

    def at_zl(d, dc):
        return (y, zh, mod(zl + d, 4), x, mod(c + dc, 2))

    def rows_of(block, first, count):
        return pl.ds(pl.multiple_of(block * 128 + first, 16), count)

    own = y * 2 + zh
    own_rows = rows_of(own, 0, 128)
    load_wq = pltpu.make_async_copy(wq_hbm, wbuf.at[own_rows, pl.ds(0, 512)], local.at[0])
    load_wo = pltpu.make_async_copy(wo_hbm, wbuf.at[own_rows, pl.ds(512, 256)], local.at[1])
    load_og = pltpu.make_async_copy(og_hbm, og, local.at[2])
    load_as = pltpu.make_async_copy(as_hbm, saved, local.at[3])
    load_hid = pltpu.make_async_copy(hid_hbm, hid, local.at[4])
    small = [
        pltpu.make_async_copy(src, dst, local.at[5 + i])
        for i, (src, dst) in enumerate(
            ((start_hbm, start_ref), (inv_hbm, inv_ref), (lse_hbm, lse_ref), (doc_hbm, doc_ref))
        )
    ]
    for copy in (load_wq, load_wo, *small, load_og, load_as, load_hid):
        copy.start()
    near = [mate, mirror]
    for at in (at_y, at_x, at_z):
        near += [at(1), at(-1)]
    barrier = pltpu.get_barrier_semaphore()

    def tell(sem, device):
        pl.semaphore_signal(sem, inc=1, device_id=device, device_id_type=MESH)

    for peer in near:
        tell(barrier, peer)

    load_wq.wait()
    load_wo.wait()
    pl.semaphore_wait(barrier, len(near))

    def hear(step):
        for i in range(4):
            pl.semaphore_wait(chain.at[step, i], 1)

    def pass_word(step):
        for i, device in enumerate((at_x(1), at_x(-1), at_z(1), at_z(-1))):
            tell(chain.at[step, i], device)

    pass_word(0)

    flags = Flags(sems)
    weights_sent = flags.take()
    rows_sent = []

    def weight(block, first, count, device, got):
        ref = wbuf.at[rows_of(block, first, count), :]
        start(ref, ref, device, weights_sent, got)
        rows_sent.append(count)

    color = lax.rem(x, 2)
    base, other_base = color * 64 + c * 32, (1 - color) * 64 + c * 32
    along_y = {s: (at_y(s), at_y(-s)) for s in (1, 2)}
    along_x = (at_x(1), at_x(-1))
    across_x = (at_x(1, 1), at_x(-1, 1))
    near_rows, third_rows, far_rows = [], [], []
    shared = [(flags.take(), near_rows)] * 3
    shared += [(flags.take(), third_rows), (flags.take(), far_rows)]

    class Ring:
        def __init__(self, zside, leap):
            self.zside, self.leap = zside, leap
            self.due = {s: {} for s in range(1, 5)}
            self.beside = {s: (flags.take(), []) for s in range(5)}
            for u in range(2):
                for w in range(2):
                    for s in (2, 1) if leap else (1,):
                        self.piece(0, u, w, s, s)

        def block(self, d):
            return mod(y + d, 8) * 2 + self.zside

        def piece(self, d, u, w, s, hop):
            self.due[s][w, u] = flags.take()
            weight(self.block(d), base + 16 * u, 16, along_y[hop][w], self.due[s][w, u])

        def hand_over(self, d, u, s):
            got, rows = self.beside[s]
            for device in (along_x[u], across_x[u]) if s == 4 else (along_x[u],):
                weight(self.block(d), base + 16 * u, 16, device, got)
                rows.append(16)

        def to_mate(self, d, first):
            got, rows = shared[abs(d)]
            weight(self.block(d), first, 32, mate, got)
            rows.append(32)

        def step(self, s):
            for (w, u), got in self.due[s].items():
                await_bytes(wbuf, 16, got)
                d = s if w else -s
                if self.leap and s == 2:
                    if u == w:
                        self.piece(d, u, w, 4, 2)
                    self.piece(d, u, w, 3, 1)
                elif not self.leap and (s < 3 or (s == 3 and u == w)):
                    self.piece(d, u, w, s + 1, 1)
                self.hand_over(d, u, s)
            self.mate_rows(s, base)

        def mate_rows(self, s, first):
            for d in {0: (0,), 4: (4,)}.get(s, (-s, s)):
                self.to_mate(d, first)

        def collect(self, s):
            got, rows = self.beside[s]
            await_bytes(wbuf, sum(rows), got)
            if s < 4:
                self.mate_rows(s, other_base)

    ring_a = Ring(zh, False)
    from_mirror = flags.take()
    weight(own, base, 32, mirror, from_mirror)

    for copy in small:
        copy.wait()
    positions = (start_ref[0] + lax.broadcasted_iota(jnp.int32, (ROWS, HEAD), 0)).astype(F32)
    angles = positions * inv_ref[...]
    sign = jnp.where(lax.broadcasted_iota(jnp.int32, (ROWS, HEAD), 1) < HEAD // 2, -1.0, 1.0)
    for h in range(2):
        lse[h] = jnp.broadcast_to(lse_ref[h : h + 1, :], (HEAD, ROWS)).T
    cos_ref[...] = jnp.cos(angles)
    sin_ref[...] = jnp.sin(angles) * sign

    def transpose(src, dst, j):
        part = src[:, 256 * j : 256 * (j + 1)].T
        for i in range(2):
            for h in range(2):
                b = 2 * j + i
                dst[h, b * 64 : (b + 1) * 64, :] = part[i * 128 + h * 64 : i * 128 + h * 64 + 64]

    sign_c = 1 - 2 * c

    class First:
        def __init__(self, chunks, parts, relay, me, at):
            self.chunks, self.parts, self.relay, self.me, self.at = chunks, parts, relay, me, at
            self.sent, self.got, self.far = flags.take(), flags.take(), flags.take()
            start(chunks.at[mod(me + 4, 8)], relay, at(sign_c), self.sent, self.far)
            for i, d in enumerate((-3, 2, -2, -1)):
                self.go(i, d)

        def go(self, i, d):
            there = mod(self.me + sign_c * d, 8)
            start(self.chunks.at[there], self.parts.at[i], self.at(sign_c * d), self.sent, self.got)

        def pass_on(self):
            await_bytes(self.chunks, 1, self.far)
            there = mod(self.me + sign_c * 3, 8)
            both = self.chunks[there].astype(F32) + self.relay[...].astype(F32)
            self.chunks[there] = both.astype(BF16)
            self.go(4, 3)
            self.go(5, 1)

        def total(self):
            await_bytes(self.chunks, 6, self.got)
            return summed(self.chunks[self.me], self.parts, 6).astype(BF16)

        def left(self):
            await_bytes(self.chunks, 7, self.sent)

    def summed(own_part, parts, count):
        total = own_part.astype(F32)
        for i in range(count):
            total = total + parts[i].astype(F32)
        return total

    def in_order(parts):
        total = parts[0].astype(F32)
        for i in range(1, 8):
            total = total + parts[i].astype(F32)
        return total

    def put_z(dst, block, tile):
        for qr in range(4):
            zz = (block % 2) * 4 + qr
            yy = block // 2
            dst[zz, yy * 16 : yy * 16 + 16, :] = tile[qr * 16 : qr * 16 + 16]

    def out_term(h, ch):
        return dot(og_t[h, ch * 256 : (ch + 1) * 256, :], saved[...])

    load_og.wait()
    load_as.wait()
    for j in range(8):
        transpose(og, og_t, j)
    for ch in range(4):
        part = out_term(1 - c, ch).astype(BF16)
        for i in range(4):
            put_z(gs_z, ch * 4 + i, part[i * 64 : i * 64 + 64])
    core_z = Batch(flags, gs_z).send(gs_z, gr_z, mate, 8)
    hear(0)
    pass_word(1)
    ring_a.step(1)
    await_bytes(wbuf, 32, from_mirror)
    ring_b = Ring(1 - zh, True)
    for u in range(2):
        ring_b.hand_over(0, u, 0)
    ring_b.mate_rows(0, base)
    hear(1)
    pass_word(2)
    for ch in range(4):
        part = out_term(c, ch)
        for i in range(4):
            put_z(s_z, ch * 4 + i, part[i * 64 : i * 64 + 64].astype(BF16))
    ring_a.step(2)
    hear(2)
    core_z.arrived()
    for k in range(8):
        s_z[k] = (s_z[k].astype(F32) + gr_z[k].astype(F32)).astype(BF16)
    first_z = First(s_z, r_z, far_z, z, at_z)
    ring_a.collect(1)
    ring_b.step(1)
    ring_b.step(2)
    ring_a.step(3)
    ring_a.collect(2)
    ring_b.collect(0)
    ring_b.collect(1)
    ring_b.step(3)
    ring_a.step(4)
    first_z.pass_on()
    load_hid.wait()
    for j in range(4):
        transpose(hid, hid_t, j)
    ring_b.step(4)
    ring_b.collect(2)
    ring_a.collect(3)
    for j in range(4, 8):
        transpose(hid, hid_t, j)
    ring_b.collect(3)
    await_bytes(wbuf, sum(near_rows), shared[0][0])

    def project(d, first=False):
        rows = pl.ds(pl.multiple_of(mod(y + d, 8) * 256, 256), 256)
        for src, cols in ((hid, slice(0, 512)), (og, slice(512, 768))):
            part = dot(src[:, rows], wbuf[rows, cols])
            proj[:, cols] = part if first else proj[:, cols] + part

    project(0, True)
    for d in (1, -1, 2, -2):
        project(d)
    await_bytes(wbuf, sum(third_rows), shared[3][0])
    for d in (3, -3):
        project(d)
    ring_a.collect(4)
    ring_b.collect(4)
    await_bytes(wbuf, sum(far_rows), shared[4][0])
    project(4)
    cosine, sines = cos_ref[...], sin_ref[...]

    def rotary(value):
        return value * cosine + pltpu.roll(value, HEAD // 2, 1) * sines

    def rotary_back(value):
        return value * cosine - pltpu.roll(value, HEAD // 2, 1) * sines

    keys = rotary(proj[:, 256:384]).astype(BF16)
    values = proj[:, 384:512].astype(BF16)
    row = lax.broadcasted_iota(jnp.int32, (ROWS, ROWS), 0)
    col = lax.broadcasted_iota(jnp.int32, (ROWS, ROWS), 1)
    allowed = col <= row
    end = jnp.int32(0)
    for i in range(4):
        end = end + doc_ref[0, i]
        allowed = allowed & ((row >= end) == (col >= end))
    scale = 1.0 / HEAD**0.5
    key_grad = jnp.zeros((ROWS, HEAD), F32)
    value_grad = jnp.zeros((ROWS, HEAD), F32)
    for h in range(2):
        lanes = slice(h * HEAD, (h + 1) * HEAD)
        query = rotary(proj[:, lanes]).astype(BF16)
        grad = proj[:, 512 + h * HEAD : 512 + (h + 1) * HEAD].astype(BF16)
        scores = dot(query, keys, ((1,), (1,))) * scale
        probs = jnp.where(allowed, jnp.exp(scores - lse[h, :, 0:1]), 0.0)
        dprobs = dot(grad, values, ((1,), (1,)))
        delta = jnp.sum(
            grad.astype(F32) * saved[:, lanes].astype(F32), axis=1, keepdims=True
        )
        dscores = (probs * (dprobs - delta) * scale).astype(BF16)
        value_grad += dot(probs.astype(BF16), grad, ((0,), (0,)))
        key_grad += dot(dscores, query, ((0,), (0,)))
        dqkv[:, lanes] = rotary_back(dot(dscores, keys)).astype(BF16)
    dqkv[:, 256:384] = rotary_back(key_grad).astype(BF16)
    dqkv[:, 384:512] = value_grad.astype(BF16)

    def y_term(h, dst):
        for ch in range(4):
            part = dot(hid_t[h, ch * 256 : (ch + 1) * 256, :], dqkv[:, :256]).astype(BF16)
            for i in range(4):
                at, side = (ch * 4 + i) // 2, (i % 2) * 64
                dst[at, side : side + 64, :] = part[i * 64 : i * 64 + 64]

    def x_term(h, dst):
        for ch in range(4):
            part = dot(hid_t[h, ch * 256 : (ch + 1) * 256, :], dqkv[:, 256:]).astype(BF16)
            for i in range(4):
                at = (ch * 4 + i) * 16
                for qr in range(4):
                    for ct in range(2):
                        dst[qr * 2 + ct, at : at + 16, :] = part[
                            i * 64 + qr * 16 : i * 64 + qr * 16 + 16, ct * 128 : ct * 128 + 128
                        ]

    def add(dst, more):
        for k in range(8):
            dst[k] = (dst[k].astype(F32) + more[k].astype(F32)).astype(BF16)

    y_term(1 - c, gs_y)
    core_y = Batch(flags, gs_y).send(gs_y, gr_y, mate, 8)
    x_term(1 - c, gs_x)
    core_x = Batch(flags, gs_x).send(gs_x, gr_x, mate, 8)
    y_term(c, s_y)
    def exchange(parts, landing, me, at):
        batch = Batch(flags, parts)
        for d in FAR_FIRST:
            batch.send(parts.at[mod(me + d, 8)], landing.at[d - 1], at(d))
        return batch

    def broadcast(pieces, me, devices):
        batch = Batch(flags, pieces)
        for device in devices:
            batch.send(pieces.at[me], pieces.at[me], device)
        return batch

    total = first_z.total()
    for k in range(8):
        s2_z[k] = total[k * 16 : k * 16 + 16]
    second_z = exchange(s2_z, r2_z, y, at_y)
    x_term(c, s_x)
    core_y.arrived()
    add(s_y, gr_y)
    first_y = First(s_y, r_y, far_y, y, at_y)
    core_x.arrived()
    add(s_x, gr_x)
    first_x = First(s_x, r_x, far_x, x, at_x)

    for n in range(4):
        cols = slice(n * 512, (n + 1) * 512)
        ig_ref[:, cols] = dot(dqkv[...], wbuf[cols, :512], ((1,), (1,))).astype(BF16)
    first_y.pass_on()
    first_x.pass_on()

    await_bytes(wbuf, sum(rows_sent), weights_sent)
    for batch in (core_z, core_y, core_x, first_z, second_z):
        batch.left()
    second_z.arrived()
    r3_z[x] = summed(s2_z[y], r2_z, 7).astype(BF16)
    third_z = broadcast(r3_z, x, [at_x(d) for d in FAR_FIRST])

    total = first_y.total()
    for k in range(8):
        s2_y[k] = total[k * 16 : k * 16 + 16]
    second_y = exchange(s2_y, r2_y, z, at_z)
    total = first_x.total()
    for k in range(8):
        s2_x[k] = total[k * 32 : k * 32 + 32]
    second_x = exchange(s2_x, r2_x, y, at_y)

    beside_zl = [at_zl(d, dc) for d in (2, 3, 1) for dc in range(2)] + [mate]
    beside_z = [at_z(d, dc) for d in FAR_FIRST for dc in range(2)] + [mate]
    beside_x = [at_x(d, dc) for d in FAR_FIRST for dc in range(2)] + [mate]

    mine = c * 4 + zl
    third_z.arrived()
    fz[mine] = in_order(r3_z).astype(BF16)
    spread = [broadcast(fz, mine, beside_zl)]

    second_y.arrived()
    r3_y[x] = summed(s2_y[z], r2_y, 7).astype(BF16)
    third_y = broadcast(r3_y, x, [at_x(d) for d in FAR_FIRST])
    second_x.arrived()
    r3_x[z] = summed(s2_x[y], r2_x, 7).astype(BF16)
    third_x = broadcast(r3_x, z, [at_z(d) for d in FAR_FIRST])

    def squares(*pieces):
        rows = [jnp.sum(piece * piece, axis=0, keepdims=True) for piece in pieces]
        lanes = [row[:, i : i + 128] for row in rows for i in range(0, row.shape[1], 128)]
        return sum(lanes[1:], lanes[0])

    first_y.left()
    first_x.left()
    third_y.arrived()
    fy[mine] = in_order(r3_y).astype(BF16)
    slot = c * 8 + z
    nz[slot] = squares(fy[mine].astype(F32), fz[mine].astype(F32))
    spread.append(broadcast(nz, slot, beside_z))
    spread.append(broadcast(fy, mine, beside_zl))
    third_x.arrived()
    tile = c * 8 + x
    both = in_order(r3_x).astype(BF16)
    s3_x[0], s3_x[1] = both[:16], both[16:]
    fx[tile] = s3_x[zh]
    nx[tile] = squares(both.astype(F32))
    spread.append(broadcast(nx, tile, beside_x))
    spread.append(broadcast(fx, tile, beside_x))
    for batch in spread:
        batch.arrived()
    total = nz[0] + nx[0]
    for i in range(1, 16):
        total = total + (nz[i] + nx[i])
    ny[y] = total
    along = broadcast(ny, y, [at_y(d) for d in FAR_FIRST])
    for i in range(8):
        grads_ref[i * 16 : i * 16 + 16, 0:256] = fy[i].astype(F32)
        grads_ref[i * 16 : i * 16 + 16, 512:768] = fz[i].astype(F32)
        for ct in range(2):
            at = (i // 4) * 8 + (i % 4) * 2 + ct
            grads_ref[i * 16 : i * 16 + 16, 256 + ct * 128 : 384 + ct * 128] = fx[at].astype(F32)
    for batch in (second_y, second_x, third_z, third_y, third_x, *spread):
        batch.left()
    along.arrived()
    total = ny[0]
    for i in range(1, 8):
        total = total + ny[i]
    norm_ref[...] = total
    along.left()
    assert flags.used <= SEMS, flags.used


def finish(ig_ref, grads_ref, tiles_ref, ig_out, update_out, norm_out, update_ref, norm_ref, sems):
    stores = [pltpu.make_async_copy(ig_ref, ig_out, sems.at[0])]
    stores[0].start()
    norm_sq = jnp.sum(tiles_ref[...], axis=1, keepdims=True)
    norm_ref[...] = jnp.sqrt(norm_sq)
    update_ref[...] = grads_ref[...] * lax.rsqrt(norm_sq / (D * 768) + 1e-06)
    stores.append(pltpu.make_async_copy(update_ref, update_out, sems.at[1]))
    stores.append(pltpu.make_async_copy(norm_ref, norm_out, sems.at[2]))
    for store in stores[1:]:
        store.start()
    for store in stores:
        store.wait()


def body(hidden_in, out_grad, attn_saved, row_lse, w_qkv, w_out_t, doc_lengths, seq_start):
    power = np.arange(HEAD // 2, dtype=np.float64) * 2.0 / HEAD
    inverse = np.tile(1000000.0 ** (-power), 2).astype(np.float32)[None, :]
    vmem = pl.BlockSpec(memory_space=pltpu.VMEM)
    hbm = pl.BlockSpec(memory_space=pl.ANY)
    half = (8, 128, 256)
    tall = (8, 256, 128)

    def bf(*shape):
        return pltpu.VMEM(shape, BF16)

    def f32(*shape):
        return pltpu.VMEM(shape, F32)

    input_grad, grads, tiles = pl.pallas_call(
        kernel,
        out_shape=(bf(ROWS, D), f32(128, 768), f32(1, 128)),
        in_specs=[hbm] * 9,
        out_specs=(vmem, vmem, vmem),
        scratch_shapes=[
            pltpu.SMEM((1,), jnp.int32),
            pltpu.SMEM((1, 4), jnp.int32),
            f32(1, HEAD),
            f32(2, ROWS),
            bf(ROWS, D),
            bf(ROWS, D),
            bf(ROWS, 256),
            bf(D, 768),
            bf(2, 1024, 256),
            bf(2, 1024, 256),
            f32(ROWS, 768),
            f32(2, ROWS, HEAD),
            f32(ROWS, HEAD),
            f32(ROWS, HEAD),
            bf(ROWS, 512),
            bf(*half),
            bf(*tall),
            bf(*half),
            bf(*half),
            bf(*tall),
            bf(*half),
            bf(*half),
            bf(*tall),
            bf(*half),
            bf(6, 128, 256),
            bf(6, 256, 128),
            bf(6, 128, 256),
            bf(8, 16, 256),
            bf(8, 32, 128),
            bf(8, 16, 256),
            bf(7, 16, 256),
            bf(7, 32, 128),
            bf(7, 16, 256),
            bf(8, 16, 256),
            bf(2, 16, 128),
            bf(8, 32, 128),
            bf(8, 16, 256),
            bf(128, 256),
            bf(256, 128),
            bf(128, 256),
            bf(8, 16, 256),
            bf(8, 16, 256),
            bf(16, 16, 128),
            f32(16, 1, 128),
            f32(16, 1, 128),
            f32(8, 1, 128),
            pltpu.SemaphoreType.DMA((SEMS,)),
            pltpu.SemaphoreType.DMA((9,)),
            pltpu.SemaphoreType.REGULAR((3, 4)),
        ],
        compiler_params=pltpu.CompilerParams(collective_id=0, has_side_effects=True),
        name="attention_backward",
    )(
        seq_start,
        doc_lengths,
        jnp.asarray(inverse),
        row_lse.T,
        hidden_in,
        out_grad,
        attn_saved,
        w_qkv,
        w_out_t,
    )
    input_grad, grad_update, norm = pl.pallas_call(
        finish,
        out_shape=(
            jax.ShapeDtypeStruct((ROWS, D), BF16),
            jax.ShapeDtypeStruct((128, 768), F32),
            jax.ShapeDtypeStruct((1, 1), F32),
        ),
        in_specs=[vmem] * 3,
        out_specs=(hbm, hbm, hbm),
        scratch_shapes=[f32(128, 768), f32(1, 1), pltpu.SemaphoreType.DMA((3,))],
        compiler_params=pltpu.CompilerParams(vmem_limit_bytes=8 * 2**20),
        name="scaled_outputs",
    )(input_grad, grads, tiles)
    return (input_grad, grad_update, norm[0, 0])


def solution(mesh):
    split = Mesh(mesh.devices.reshape(8, 2, 4, 8, 2), AXES)
    tokens = P(FSDP_REP, None)
    in_specs = (tokens, tokens, tokens, tokens, P(FSDP, None), P(FSDP, None), tokens, P(FSDP_REP))
    out_specs = (tokens, P(FSDP, None), P())
    return jax.shard_map(body, mesh=split, in_specs=in_specs, out_specs=out_specs, check_vma=False)
```

```python
import jax
import jax.numpy as jnp
import numpy as np
from jax import lax
from jax.experimental import pallas as pl
from jax.experimental.pallas import tpu as pltpu
from jax.sharding import Mesh
from jax.sharding import PartitionSpec as P

D = 2048
HEAD = 128
ROWS = 256
AXES = ("fsdp_0", "fsdp_1", "rep_0", "rep_1", "rep_2")
FSDP = AXES[:2]
FSDP_REP = AXES
F32 = jnp.float32
BF16 = jnp.bfloat16
SEMS = 82
FAR_FIRST = (4, 3, 5, 2, 6, 1, 7)


def mod(value, size):
    return lax.rem(value + size, size)


def dot(left, right, contract=((1,), (0,))):
    return lax.dot_general(left, right, (contract, ((), ())), preferred_element_type=F32)


MESH = pl.DeviceIdType.MESH


class Flags:
    def __init__(self, sems):
        self.sems, self.used = sems, 0

    def take(self):
        self.used += 1
        return self.sems.at[self.used - 1]


def start(src, dst, device, sent, got):
    pltpu.make_async_remote_copy(
        src_ref=src, dst_ref=dst, send_sem=sent, recv_sem=got, device_id=device, device_id_type=MESH
    ).start()


def await_bytes(whole, count, flag):
    ref = whole.at[pl.ds(0, count)]
    pltpu.make_async_copy(ref, ref, flag).wait()


class Batch:
    def __init__(self, flags, whole):
        self.whole, self.sent, self.got, self.count = whole, flags.take(), flags.take(), 0

    def send(self, src, dst, device, units=1):
        start(src, dst, device, self.sent, self.got)
        self.count += units
        return self

    def arrived(self):
        await_bytes(self.whole, self.count, self.got)

    def left(self):
        await_bytes(self.whole, self.count, self.sent)


def kernel(
    start_hbm,
    doc_hbm,
    inv_hbm,
    lse_hbm,
    hid_hbm,
    og_hbm,
    as_hbm,
    wq_hbm,
    wo_hbm,
    ig_ref,
    grads_ref,
    norm_ref,
    start_ref,
    doc_ref,
    inv_ref,
    lse_ref,
    hid,
    og,
    saved,
    wbuf,
    hid_t,
    og_t,
    proj,
    lse,
    cos_ref,
    sin_ref,
    dqkv,
    gs_y,
    gs_x,
    gs_z,
    gr_y,
    gr_x,
    gr_z,
    s_y,
    s_x,
    s_z,
    r_y,
    r_x,
    r_z,
    s2_y,
    s2_x,
    s2_z,
    r2_y,
    r2_x,
    r2_z,
    r3_y,
    s3_x,
    r3_x,
    r3_z,
    far_y,
    far_x,
    far_z,
    fy,
    fz,
    fx,
    nz,
    nx,
    ny,
    sems,
    local,
    chain,
):
    y = lax.axis_index(AXES[0])
    zh = lax.axis_index(AXES[1])
    zl = lax.axis_index(AXES[2])
    x = lax.axis_index(AXES[3])
    c = lax.axis_index(AXES[4])
    z = zh * 4 + zl
    mate = (y, zh, zl, x, 1 - c)
    mirror = (y, 1 - zh, 3 - zl, x, c)

    def at_y(d):
        return (mod(y + d, 8), zh, zl, x, c)

    def at_x(d, dc=0):
        return (y, zh, zl, mod(x + d, 8), mod(c + dc, 2))

    def at_z(d, dc=0):
        there = mod(z + d, 8)
        return (y, there // 4, lax.rem(there, 4), x, mod(c + dc, 2))

    def at_zl(d, dc):
        return (y, zh, mod(zl + d, 4), x, mod(c + dc, 2))

    def rows_of(block, first, count):
        return pl.ds(pl.multiple_of(block * 128 + first, 16), count)

    own = y * 2 + zh
    own_rows = rows_of(own, 0, 128)
    load_wq = pltpu.make_async_copy(wq_hbm, wbuf.at[own_rows, pl.ds(0, 512)], local.at[0])
    load_wo = pltpu.make_async_copy(wo_hbm, wbuf.at[own_rows, pl.ds(512, 256)], local.at[1])
    load_og = pltpu.make_async_copy(og_hbm, og, local.at[2])
    load_as = pltpu.make_async_copy(as_hbm, saved, local.at[3])
    load_hid = pltpu.make_async_copy(hid_hbm, hid, local.at[4])
    small = [
        pltpu.make_async_copy(src, dst, local.at[5 + i])
        for i, (src, dst) in enumerate(
            ((start_hbm, start_ref), (inv_hbm, inv_ref), (lse_hbm, lse_ref), (doc_hbm, doc_ref))
        )
    ]
    for copy in (load_wq, load_wo, *small, load_og, load_as, load_hid):
        copy.start()
    near = [mate, mirror]
    for at in (at_y, at_x, at_z):
        near += [at(1), at(-1)]
    barrier = pltpu.get_barrier_semaphore()

    def tell(sem, device):
        pl.semaphore_signal(sem, inc=1, device_id=device, device_id_type=MESH)

    for peer in near:
        tell(barrier, peer)

    load_wq.wait()
    load_wo.wait()
    pl.semaphore_wait(barrier, len(near))

    def hear(step):
        for i in range(4):
            pl.semaphore_wait(chain.at[step, i], 1)

    def pass_word(step):
        for i, device in enumerate((at_x(1), at_x(-1), at_z(1), at_z(-1))):
            tell(chain.at[step, i], device)

    pass_word(0)

    flags = Flags(sems)
    weights_sent = flags.take()
    rows_sent = []

    def weight(block, first, count, device, got):
        ref = wbuf.at[rows_of(block, first, count), :]
        start(ref, ref, device, weights_sent, got)
        rows_sent.append(count)

    color = lax.rem(x, 2)
    base, other_base = color * 64 + c * 32, (1 - color) * 64 + c * 32
    along_y = {s: (at_y(s), at_y(-s)) for s in (1, 2)}
    along_x = (at_x(1), at_x(-1))
    across_x = (at_x(1, 1), at_x(-1, 1))
    near_rows, third_rows, far_rows = [], [], []
    shared = [(flags.take(), near_rows)] * 3
    shared += [(flags.take(), third_rows), (flags.take(), far_rows)]

    class Ring:
        def __init__(self, zside, leap):
            self.zside, self.leap = zside, leap
            self.due = {s: {} for s in range(1, 5)}
            self.beside = {s: (flags.take(), []) for s in range(5)}
            for u in range(2):
                for w in range(2):
                    for s in (2, 1) if leap else (1,):
                        self.piece(0, u, w, s, s)

        def block(self, d):
            return mod(y + d, 8) * 2 + self.zside

        def piece(self, d, u, w, s, hop):
            self.due[s][w, u] = flags.take()
            weight(self.block(d), base + 16 * u, 16, along_y[hop][w], self.due[s][w, u])

        def hand_over(self, d, u, s):
            got, rows = self.beside[s]
            for device in (along_x[u], across_x[u]) if self.direct(s) else (along_x[u],):
                weight(self.block(d), base + 16 * u, 16, device, got)
                rows.append(16)

        def direct(self, s):
            return self.leap and s == 4

        def to_mate(self, d, first):
            got, rows = shared[abs(d)]
            weight(self.block(d), first, 32, mate, got)
            rows.append(32)

        def step(self, s):
            for (w, u), got in self.due[s].items():
                await_bytes(wbuf, 16, got)
                d = s if w else -s
                if self.leap and s == 2:
                    if u == w:
                        self.piece(d, u, w, 4, 2)
                    self.piece(d, u, w, 3, 1)
                elif not self.leap and (s < 3 or (s == 3 and u == w)):
                    self.piece(d, u, w, s + 1, 1)
                self.hand_over(d, u, s)
            self.mate_rows(s, base)

        def mate_rows(self, s, first):
            for d in {0: (0,), 4: (4,)}.get(s, (-s, s)):
                self.to_mate(d, first)

        def collect(self, s):
            got, rows = self.beside[s]
            await_bytes(wbuf, sum(rows), got)
            if not self.direct(s):
                self.mate_rows(s, other_base)

    ring_a = Ring(zh, False)
    from_mirror = flags.take()
    weight(own, base, 32, mirror, from_mirror)

    for copy in small:
        copy.wait()
    positions = (start_ref[0] + lax.broadcasted_iota(jnp.int32, (ROWS, HEAD), 0)).astype(F32)
    angles = positions * inv_ref[...]
    sign = jnp.where(lax.broadcasted_iota(jnp.int32, (ROWS, HEAD), 1) < HEAD // 2, -1.0, 1.0)
    for h in range(2):
        lse[h] = jnp.broadcast_to(lse_ref[h : h + 1, :], (HEAD, ROWS)).T
    cos_ref[...] = jnp.cos(angles)
    sin_ref[...] = jnp.sin(angles) * sign

    def transpose(src, dst, j):
        part = src[:, 256 * j : 256 * (j + 1)].T
        for i in range(2):
            for h in range(2):
                b = 2 * j + i
                dst[h, b * 64 : (b + 1) * 64, :] = part[i * 128 + h * 64 : i * 128 + h * 64 + 64]

    sign_c = 1 - 2 * c

    class First:
        def __init__(self, chunks, parts, relay, me, at):
            self.chunks, self.parts, self.relay, self.me, self.at = chunks, parts, relay, me, at
            self.sent, self.got, self.far = flags.take(), flags.take(), flags.take()
            start(chunks.at[mod(me + 4, 8)], relay, at(sign_c), self.sent, self.far)
            for i, d in enumerate((-3, 2, -2, -1)):
                self.go(i, d)

        def go(self, i, d):
            there = mod(self.me + sign_c * d, 8)
            start(self.chunks.at[there], self.parts.at[i], self.at(sign_c * d), self.sent, self.got)

        def pass_on(self):
            await_bytes(self.chunks, 1, self.far)
            there = mod(self.me + sign_c * 3, 8)
            both = self.chunks[there].astype(F32) + self.relay[...].astype(F32)
            self.chunks[there] = both.astype(BF16)
            self.go(4, 3)
            self.go(5, 1)

        def total(self):
            await_bytes(self.chunks, 6, self.got)
            return summed(self.chunks[self.me], self.parts, 6).astype(BF16)

        def left(self):
            await_bytes(self.chunks, 7, self.sent)

    def summed(own_part, parts, count):
        total = own_part.astype(F32)
        for i in range(count):
            total = total + parts[i].astype(F32)
        return total

    def in_order(parts):
        total = parts[0].astype(F32)
        for i in range(1, 8):
            total = total + parts[i].astype(F32)
        return total

    def put_z(dst, block, tile):
        for qr in range(4):
            zz = (block % 2) * 4 + qr
            yy = block // 2
            dst[zz, yy * 16 : yy * 16 + 16, :] = tile[qr * 16 : qr * 16 + 16]

    def out_term(h, ch):
        return dot(og_t[h, ch * 256 : (ch + 1) * 256, :], saved[...])

    load_og.wait()
    load_as.wait()
    for j in range(8):
        transpose(og, og_t, j)
    for ch in range(4):
        part = out_term(1 - c, ch).astype(BF16)
        for i in range(4):
            put_z(gs_z, ch * 4 + i, part[i * 64 : i * 64 + 64])
    core_z = Batch(flags, gs_z).send(gs_z, gr_z, mate, 8)
    hear(0)
    pass_word(1)
    ring_a.step(1)
    await_bytes(wbuf, 32, from_mirror)
    ring_b = Ring(1 - zh, True)
    for u in range(2):
        ring_b.hand_over(0, u, 0)
    ring_b.mate_rows(0, base)
    hear(1)
    pass_word(2)
    for ch in range(4):
        part = out_term(c, ch)
        for i in range(4):
            put_z(s_z, ch * 4 + i, part[i * 64 : i * 64 + 64].astype(BF16))
    ring_a.step(2)
    hear(2)
    core_z.arrived()
    for k in range(8):
        s_z[k] = (s_z[k].astype(F32) + gr_z[k].astype(F32)).astype(BF16)
    first_z = First(s_z, r_z, far_z, z, at_z)
    ring_a.collect(1)
    ring_b.step(1)
    ring_b.step(2)
    ring_a.step(3)
    ring_a.collect(2)
    ring_b.collect(0)
    ring_b.collect(1)
    ring_b.step(3)
    ring_a.step(4)
    first_z.pass_on()
    load_hid.wait()
    for j in range(4):
        transpose(hid, hid_t, j)
    ring_b.step(4)
    ring_b.collect(2)
    ring_a.collect(3)
    for j in range(4, 8):
        transpose(hid, hid_t, j)
    ring_b.collect(3)
    ring_a.collect(4)
    await_bytes(wbuf, sum(near_rows), shared[0][0])

    def project(d, first=False):
        rows = pl.ds(pl.multiple_of(mod(y + d, 8) * 256, 256), 256)
        for src, cols in ((hid, slice(0, 512)), (og, slice(512, 768))):
            part = dot(src[:, rows], wbuf[rows, cols])
            proj[:, cols] = part if first else proj[:, cols] + part

    project(0, True)
    for d in (1, -1, 2, -2):
        project(d)
    await_bytes(wbuf, sum(third_rows), shared[3][0])
    for d in (3, -3):
        project(d)
    ring_b.collect(4)
    await_bytes(wbuf, sum(far_rows), shared[4][0])
    project(4)
    cosine, sines = cos_ref[...], sin_ref[...]

    def rotary(value):
        return value * cosine + pltpu.roll(value, HEAD // 2, 1) * sines

    def rotary_back(value):
        return value * cosine - pltpu.roll(value, HEAD // 2, 1) * sines

    keys = rotary(proj[:, 256:384]).astype(BF16)
    values = proj[:, 384:512].astype(BF16)
    row = lax.broadcasted_iota(jnp.int32, (ROWS, ROWS), 0)
    col = lax.broadcasted_iota(jnp.int32, (ROWS, ROWS), 1)
    allowed = col <= row
    end = jnp.int32(0)
    for i in range(4):
        end = end + doc_ref[0, i]
        allowed = allowed & ((row >= end) == (col >= end))
    scale = 1.0 / HEAD**0.5
    key_grad = jnp.zeros((ROWS, HEAD), F32)
    value_grad = jnp.zeros((ROWS, HEAD), F32)
    for h in range(2):
        lanes = slice(h * HEAD, (h + 1) * HEAD)
        query = rotary(proj[:, lanes]).astype(BF16)
        grad = proj[:, 512 + h * HEAD : 512 + (h + 1) * HEAD].astype(BF16)
        scores = dot(query, keys, ((1,), (1,))) * scale
        probs = jnp.where(allowed, jnp.exp(scores - lse[h, :, 0:1]), 0.0)
        dprobs = dot(grad, values, ((1,), (1,)))
        delta = jnp.sum(
            grad.astype(F32) * saved[:, lanes].astype(F32), axis=1, keepdims=True
        )
        dscores = (probs * (dprobs - delta) * scale).astype(BF16)
        value_grad += dot(probs.astype(BF16), grad, ((0,), (0,)))
        key_grad += dot(dscores, query, ((0,), (0,)))
        dqkv[:, lanes] = rotary_back(dot(dscores, keys)).astype(BF16)
    dqkv[:, 256:384] = rotary_back(key_grad).astype(BF16)
    dqkv[:, 384:512] = value_grad.astype(BF16)

    def y_term(h, dst):
        for ch in range(4):
            part = dot(hid_t[h, ch * 256 : (ch + 1) * 256, :], dqkv[:, :256]).astype(BF16)
            for i in range(4):
                at, side = (ch * 4 + i) // 2, (i % 2) * 64
                dst[at, side : side + 64, :] = part[i * 64 : i * 64 + 64]

    def x_term(h, dst):
        for ch in range(4):
            part = dot(hid_t[h, ch * 256 : (ch + 1) * 256, :], dqkv[:, 256:]).astype(BF16)
            for i in range(4):
                at = (ch * 4 + i) * 16
                for qr in range(4):
                    for ct in range(2):
                        dst[qr * 2 + ct, at : at + 16, :] = part[
                            i * 64 + qr * 16 : i * 64 + qr * 16 + 16, ct * 128 : ct * 128 + 128
                        ]

    def add(dst, more):
        for k in range(8):
            dst[k] = (dst[k].astype(F32) + more[k].astype(F32)).astype(BF16)

    y_term(1 - c, gs_y)
    core_y = Batch(flags, gs_y).send(gs_y, gr_y, mate, 8)
    x_term(1 - c, gs_x)
    core_x = Batch(flags, gs_x).send(gs_x, gr_x, mate, 8)
    y_term(c, s_y)
    def exchange(parts, landing, me, at):
        batch = Batch(flags, parts)
        for d in FAR_FIRST:
            batch.send(parts.at[mod(me + d, 8)], landing.at[d - 1], at(d))
        return batch

    def broadcast(pieces, me, devices):
        batch = Batch(flags, pieces)
        for device in devices:
            batch.send(pieces.at[me], pieces.at[me], device)
        return batch

    total = first_z.total()
    for k in range(8):
        s2_z[k] = total[k * 16 : k * 16 + 16]
    second_z = exchange(s2_z, r2_z, y, at_y)
    x_term(c, s_x)
    core_y.arrived()
    add(s_y, gr_y)
    first_y = First(s_y, r_y, far_y, y, at_y)
    core_x.arrived()
    add(s_x, gr_x)
    first_x = First(s_x, r_x, far_x, x, at_x)

    for n in range(4):
        cols = slice(n * 512, (n + 1) * 512)
        ig_ref[:, cols] = dot(dqkv[...], wbuf[cols, :512], ((1,), (1,))).astype(BF16)
    first_y.pass_on()
    first_x.pass_on()

    await_bytes(wbuf, sum(rows_sent), weights_sent)
    for batch in (core_z, core_y, core_x, first_z, second_z):
        batch.left()
    second_z.arrived()
    r3_z[x] = summed(s2_z[y], r2_z, 7).astype(BF16)
    third_z = broadcast(r3_z, x, [at_x(d) for d in FAR_FIRST])

    total = first_y.total()
    for k in range(8):
        s2_y[k] = total[k * 16 : k * 16 + 16]
    second_y = exchange(s2_y, r2_y, z, at_z)
    total = first_x.total()
    for k in range(8):
        s2_x[k] = total[k * 32 : k * 32 + 32]
    second_x = exchange(s2_x, r2_x, y, at_y)

    beside_zl = [at_zl(d, dc) for d in (2, 3, 1) for dc in range(2)] + [mate]
    beside_z = [at_z(d, dc) for d in FAR_FIRST for dc in range(2)] + [mate]
    beside_x = [at_x(d, dc) for d in FAR_FIRST for dc in range(2)] + [mate]

    mine = c * 4 + zl
    third_z.arrived()
    fz[mine] = in_order(r3_z).astype(BF16)
    spread = [broadcast(fz, mine, beside_zl)]

    second_y.arrived()
    r3_y[x] = summed(s2_y[z], r2_y, 7).astype(BF16)
    third_y = broadcast(r3_y, x, [at_x(d) for d in FAR_FIRST])
    second_x.arrived()
    r3_x[z] = summed(s2_x[y], r2_x, 7).astype(BF16)
    third_x = broadcast(r3_x, z, [at_z(d) for d in FAR_FIRST])

    def squares(*pieces):
        rows = [jnp.sum(piece * piece, axis=0, keepdims=True) for piece in pieces]
        lanes = [row[:, i : i + 128] for row in rows for i in range(0, row.shape[1], 128)]
        return sum(lanes[1:], lanes[0])

    first_y.left()
    first_x.left()
    third_y.arrived()
    fy[mine] = in_order(r3_y).astype(BF16)
    slot = c * 8 + z
    nz[slot] = squares(fy[mine].astype(F32), fz[mine].astype(F32))
    spread.append(broadcast(nz, slot, beside_z))
    spread.append(broadcast(fy, mine, beside_zl))
    third_x.arrived()
    tile = c * 8 + x
    both = in_order(r3_x).astype(BF16)
    s3_x[0], s3_x[1] = both[:16], both[16:]
    fx[tile] = s3_x[zh]
    nx[tile] = squares(both.astype(F32))
    spread.append(broadcast(nx, tile, beside_x))
    spread.append(broadcast(fx, tile, beside_x))
    from_z, from_x = spread[1], spread[3]
    from_z.arrived()
    from_x.arrived()
    total = nz[0] + nx[0]
    for i in range(1, 16):
        total = total + (nz[i] + nx[i])
    ny[y] = total
    along = broadcast(ny, y, [at_y(d) for d in FAR_FIRST])
    for batch in (spread[0], spread[2], spread[4]):
        batch.arrived()
    for i in range(8):
        grads_ref[i * 16 : i * 16 + 16, 0:256] = fy[i].astype(F32)
        grads_ref[i * 16 : i * 16 + 16, 512:768] = fz[i].astype(F32)
        for ct in range(2):
            at = (i // 4) * 8 + (i % 4) * 2 + ct
            grads_ref[i * 16 : i * 16 + 16, 256 + ct * 128 : 384 + ct * 128] = fx[at].astype(F32)
    for batch in (second_y, second_x, third_z, third_y, third_x, *spread):
        batch.left()
    along.arrived()
    total = ny[0]
    for i in range(1, 8):
        total = total + ny[i]
    norm_ref[...] = total
    along.left()
    assert flags.used <= SEMS, flags.used


def finish(ig_ref, grads_ref, tiles_ref, ig_out, update_out, norm_out, update_ref, norm_ref, sems):
    stores = [pltpu.make_async_copy(ig_ref, ig_out, sems.at[0])]
    stores[0].start()
    norm_sq = jnp.sum(tiles_ref[...], axis=1, keepdims=True)
    norm_ref[...] = jnp.sqrt(norm_sq)
    update_ref[...] = grads_ref[...] * lax.rsqrt(norm_sq / (D * 768) + 1e-06)
    stores.append(pltpu.make_async_copy(update_ref, update_out, sems.at[1]))
    stores.append(pltpu.make_async_copy(norm_ref, norm_out, sems.at[2]))
    for store in stores[1:]:
        store.start()
    for store in stores:
        store.wait()


def body(hidden_in, out_grad, attn_saved, row_lse, w_qkv, w_out_t, doc_lengths, seq_start):
    power = np.arange(HEAD // 2, dtype=np.float64) * 2.0 / HEAD
    inverse = np.tile(1000000.0 ** (-power), 2).astype(np.float32)[None, :]
    vmem = pl.BlockSpec(memory_space=pltpu.VMEM)
    hbm = pl.BlockSpec(memory_space=pl.ANY)
    half = (8, 128, 256)
    tall = (8, 256, 128)

    def bf(*shape):
        return pltpu.VMEM(shape, BF16)

    def f32(*shape):
        return pltpu.VMEM(shape, F32)

    input_grad, grads, tiles = pl.pallas_call(
        kernel,
        out_shape=(bf(ROWS, D), f32(128, 768), f32(1, 128)),
        in_specs=[hbm] * 9,
        out_specs=(vmem, vmem, vmem),
        scratch_shapes=[
            pltpu.SMEM((1,), jnp.int32),
            pltpu.SMEM((1, 4), jnp.int32),
            f32(1, HEAD),
            f32(2, ROWS),
            bf(ROWS, D),
            bf(ROWS, D),
            bf(ROWS, 256),
            bf(D, 768),
            bf(2, 1024, 256),
            bf(2, 1024, 256),
            f32(ROWS, 768),
            f32(2, ROWS, HEAD),
            f32(ROWS, HEAD),
            f32(ROWS, HEAD),
            bf(ROWS, 512),
            bf(*half),
            bf(*tall),
            bf(*half),
            bf(*half),
            bf(*tall),
            bf(*half),
            bf(*half),
            bf(*tall),
            bf(*half),
            bf(6, 128, 256),
            bf(6, 256, 128),
            bf(6, 128, 256),
            bf(8, 16, 256),
            bf(8, 32, 128),
            bf(8, 16, 256),
            bf(7, 16, 256),
            bf(7, 32, 128),
            bf(7, 16, 256),
            bf(8, 16, 256),
            bf(2, 16, 128),
            bf(8, 32, 128),
            bf(8, 16, 256),
            bf(128, 256),
            bf(256, 128),
            bf(128, 256),
            bf(8, 16, 256),
            bf(8, 16, 256),
            bf(16, 16, 128),
            f32(16, 1, 128),
            f32(16, 1, 128),
            f32(8, 1, 128),
            pltpu.SemaphoreType.DMA((SEMS,)),
            pltpu.SemaphoreType.DMA((9,)),
            pltpu.SemaphoreType.REGULAR((3, 4)),
        ],
        compiler_params=pltpu.CompilerParams(collective_id=0, has_side_effects=True),
        name="attention_backward",
    )(
        seq_start,
        doc_lengths,
        jnp.asarray(inverse),
        row_lse.T,
        hidden_in,
        out_grad,
        attn_saved,
        w_qkv,
        w_out_t,
    )
    input_grad, grad_update, norm = pl.pallas_call(
        finish,
        out_shape=(
            jax.ShapeDtypeStruct((ROWS, D), BF16),
            jax.ShapeDtypeStruct((128, 768), F32),
            jax.ShapeDtypeStruct((1, 1), F32),
        ),
        in_specs=[vmem] * 3,
        out_specs=(hbm, hbm, hbm),
        scratch_shapes=[f32(128, 768), f32(1, 1), pltpu.SemaphoreType.DMA((3,))],
        compiler_params=pltpu.CompilerParams(vmem_limit_bytes=8 * 2**20),
        name="scaled_outputs",
    )(input_grad, grads, tiles)
    return (input_grad, grad_update, norm[0, 0])


def solution(mesh):
    split = Mesh(mesh.devices.reshape(8, 2, 4, 8, 2), AXES)
    tokens = P(FSDP_REP, None)
    in_specs = (tokens, tokens, tokens, tokens, P(FSDP, None), P(FSDP, None), tokens, P(FSDP_REP))
    out_specs = (tokens, P(FSDP, None), P())
    return jax.shard_map(body, mesh=split, in_specs=in_specs, out_specs=out_specs, check_vma=False)
```
